8 devices in a mesh: task: 1 (over z), row: 8 (over y, x, core).
Axes of the slice: x: 2, y: 2, z: 1, core: 2. Of those that a mesh axis runs over, the one named last changes fastest.
Arguments:
- points: bfloat16 [24576, 512], P(('task', 'row'))
- vectors: bfloat16 [24576, 64], P(('task', 'row'))
- length_scale: float32 [1], P('task')
- out_scale: float32 [1], P('task')
Outputs:
- output: float32 [24576, 64], P(('task', 'row'))
All inputs are finite; a program needn't handle non-finite values.
Results may differ from the reference program's by a relative error of at most 0.001.
Values are sent between devices in bfloat16 or wider.
A program may use at most 1 GiB of HBM per device.

```python
import jax
import jax.numpy as jnp
from jax import lax

ROWS_DEV = 3072
GROUP = 8
FEAT = 512
COLS = 64
N_POINTS = GROUP * ROWS_DEV


def setup_inputs(seed: int = 0, part: int = 0) -> dict:
    base_key = jax.random.fold_in(jax.random.key(seed), part)
    key_x, key_o, key_m, key_v, key_l, key_s = jax.random.split(base_key, 6)
    base_pts = jax.random.normal(key_x, (GROUP, ROWS_DEV, FEAT), jnp.float32)
    offset = 1.6 * jax.random.normal(key_o, (GROUP, 1, FEAT), jnp.float32)
    points = (base_pts + offset).reshape(N_POINTS, FEAT).astype(jnp.bfloat16)
    block_mean = jax.random.normal(key_m, (GROUP, 1, COLS), jnp.float32)
    block_mean = block_mean - jnp.mean(block_mean, axis=0, keepdims=True)
    noise_val = 0.5 * jax.random.normal(key_v, (GROUP, ROWS_DEV, COLS), jnp.float32)
    vectors = (block_mean + noise_val).reshape(N_POINTS, COLS).astype(jnp.bfloat16)
    ell_ratio = jax.random.uniform(key_l, (1,), jnp.float32, 0.8, 1.25)
    length_scale = jnp.sqrt(2.0 * FEAT * ell_ratio)
    out_scale = jax.random.uniform(key_s, (1,), jnp.float32, 1.0, 2.0) / ROWS_DEV
    return {"points": points, "vectors": vectors, "length_scale": length_scale, "out_scale": out_scale}


def kernel_tile(x_rows, x_cols, length_scale, out_scale):
    norm_rows = jnp.sum(jnp.square(x_rows.astype(jnp.float32)), axis=1)
    norm_cols = jnp.sum(jnp.square(x_cols.astype(jnp.float32)), axis=1)
    gram_mat = jnp.dot(x_rows, x_cols.T, preferred_element_type=jnp.float32)
    sq_dist = jnp.maximum(norm_rows[:, None] + norm_cols[None, :] - 2.0 * gram_mat, 0.0)
    return (out_scale * jnp.exp(-sq_dist / (2.0 * length_scale * length_scale))).astype(jnp.bfloat16)


def kernel_apply(points, vectors, length_scale, out_scale):
    x_blocks = points.reshape(GROUP, ROWS_DEV, FEAT)
    v_blocks = vectors.reshape(GROUP, ROWS_DEV, COLS)

    def row_block(x_rows):
        def col_step(running, col_pair):
            x_cols, v_cols = col_pair
            kern_tile = kernel_tile(x_rows, x_cols, length_scale, out_scale)
            return running + jnp.dot(kern_tile, v_cols, preferred_element_type=jnp.float32), None

        running, _ = lax.scan(col_step, jnp.zeros((ROWS_DEV, COLS), jnp.float32), (x_blocks, v_blocks))
        return running

    return lax.map(row_block, x_blocks).reshape(N_POINTS, COLS)


def reference(points, vectors, length_scale, out_scale):
    first_pass = kernel_apply(points, vectors, length_scale, out_scale).astype(jnp.bfloat16)
    return kernel_apply(points, first_pass, length_scale, out_scale)
```

```python
import functools
import math

import jax
import jax.numpy as jnp
from jax import lax
from jax.experimental import pallas as pl
from jax.experimental.pallas import tpu as pltpu
from jax.sharding import PartitionSpec as P

MESH = pl.DeviceIdType.MESH
T = 256
FEAT = 512
COLS = 64
NCH = 12
NREL = 8
STEPS = NREL * NCH
PIECE = 64
NP = T // PIECE
NI = NCH // 2
RES_IN, RES_OF = 3, 8
N_RES = (STEPS - 24) // RES_OF * RES_IN
RING = 5
N_STREAM = STEPS - N_RES
XR = 3


def chunk_of(s):
    j = lax.rem(s + 2, 4)
    v = lax.div(s - 22, 4) - 1
    late = jnp.where(s < 26, 0, jnp.where(s >= 94, 1, lax.div(j, 2)))
    group = jnp.where(s < 26, 0, jnp.where(s >= 94, 17, v + 1 - late))
    side = lax.rem(s, 2)
    far = group >= 12
    rel = jnp.where(far, 6, 2 + 2 * side) + late
    chunk = jnp.where(far, 2 * (group - 12) + side, group)
    near_rel = lax.div(s, NCH)
    near_chunk = lax.rem(s, NCH)
    return jnp.where(s < 24, near_rel, rel), jnp.where(s < 24, near_chunk, chunk)


def stream_of(s):
    u = jnp.maximum(s - 24, 0)
    w = lax.rem(u, RES_OF)
    o = lax.div(u, RES_OF)
    streamed = jnp.logical_or(s < 24, w >= RES_IN)
    number = jnp.where(s < 24, s, 24 + o * (RES_OF - RES_IN) + w - RES_IN)
    slot = jnp.where(streamed, N_RES + lax.rem(number, RING), o * RES_IN + w)
    return streamed, number, slot


def body(
    x_hbm, vt_hbm, ls_ref, os_ref,
    out_ref, xall, kst,
    xt, vt, yall, kbuf, xr, nj, ni,
    ld_sem, kw_sem, kr_sem, vl_sem,
    rx_sem, rv_sem, so_x, so_v, sp_x, sp_v, sn_x, sn_v, ys_sem, yr_sem,
    ysum,
):
    me = lax.axis_index("row")
    partner = me + 1 - 2 * lax.rem(me, 2)
    nbr_x = me + 2 - 4 * lax.rem(lax.div(me, 2), 2)
    nbr_y = me + 4 - 8 * lax.div(me, 4)

    def remote(src, dst, ss, rs, dev):
        return pltpu.make_async_remote_copy(
            src_ref=src, dst_ref=dst, send_sem=ss, recv_sem=rs, device_id={"row": dev}, device_id_type=MESH
        )

    def send_own(k, which, dev):
        slot = (1, 2, 4)[which]
        return (
            remote(x_hbm.at[k], xall.at[slot, k], so_x.at[which, k], rx_sem.at[slot, k], dev),
            remote(vt_hbm.at[k], vt.at[slot, k], so_v.at[which, k], rv_sem.at[slot, k], dev),
        )

    def forward_partner(rel, k):
        row = lax.div(rel, 2) - 1
        return (
            remote(xall.at[rel, k], xall.at[rel + 1, k], sp_x.at[row, k], rx_sem.at[rel + 1, k], partner),
            remote(vt.at[rel, k], vt.at[rel + 1, k], sp_v.at[row, k], rv_sem.at[rel + 1, k], partner),
        )

    def forward_nbr(rel, k, dev):
        return (
            remote(xall.at[rel, k], xall.at[6, k], sn_x.at[k], rx_sem.at[6, k], dev),
            remote(vt.at[rel, k], vt.at[6, k], sn_v.at[k], rv_sem.at[6, k], dev),
        )

    barrier = pltpu.get_barrier_semaphore()
    for dev in (partner, nbr_x, nbr_y):
        pl.semaphore_signal(barrier, inc=1, device_id={"row": dev}, device_id_type=MESH)

    own_v = pltpu.make_async_copy(vt_hbm, vt.at[0], vl_sem)
    own_v.start()

    def load_own(k, slot):
        return pltpu.make_async_copy(x_hbm.at[k], xr.at[slot], ld_sem.at[slot])

    load_own(0, 0).start()
    pl.semaphore_wait(barrier, 3)

    @pl.loop(0, NCH)
    def _(k):
        for which, dev in enumerate((partner, nbr_x, nbr_y)):
            for copy in send_own(k, which, dev):
                copy.start()

    load_own(1, 1).start()

    @pl.loop(0, NCH)
    def _(k):
        slot = lax.rem(k, 2)
        load_own(k, slot).wait()
        norm = jnp.zeros((1, T), jnp.float32)
        for h in range(2):
            part = xr[slot, :, h * T : (h + 1) * T].astype(jnp.float32).T
            norm = norm + jnp.sum(part * part, axis=0, keepdims=True)
            xt[k, h * T : (h + 1) * T, :] = (part * -2.0).astype(jnp.bfloat16)
        ni[k] = jnp.broadcast_to(norm, (8, T))

        @pl.when(k + 2 < NCH)
        def _():
            load_own(k + 2, slot).start()

    own_v.wait()
    load_own(0, 0).start()

    scale = jnp.full((1, T), ls_ref[0], jnp.float32)
    rate = -math.log2(math.e) / (2.0 * scale * scale)
    amp = jnp.full((1, T), os_ref[0], jnp.float32)

    @pl.loop(0, NCH)
    def _(k):
        ysum[k] = jnp.zeros((COLS, T), jnp.float32)

    def write_k(number):
        slot = lax.rem(number, RING)
        return pltpu.make_async_copy(kbuf.at[N_RES + slot], kst.at[number], kw_sem.at[slot])

    def read_k(number):
        slot = lax.rem(number, RING)
        return pltpu.make_async_copy(kst.at[number], kbuf.at[N_RES + slot], kr_sem.at[slot])

    def tile(x_slot, k_slot, n_slot, i):
        gram_tile = jnp.dot(
            xr[x_slot], xt[i], preferred_element_type=jnp.float32
        )
        dist = jnp.maximum((nj[n_slot] + ni[i, 0:1, :]) + gram_tile, 0.0)
        kbuf[k_slot, i] = (amp * jnp.exp2(dist * rate)).astype(jnp.bfloat16)

    def apply(k_slot, lhs, i):
        ysum[i] += jnp.dot(lhs, kbuf[k_slot, i], preferred_element_type=jnp.float32)

    def fetch(s):
        rel, k = chunk_of(s)
        slot = lax.rem(s, XR)

        @pl.when(rel == 0)
        def _():
            load_own(k, slot).start()

        @pl.when(rel > 0)
        def _():
            remote(xall.at[rel, k], xall.at[rel, k], so_x.at[0, 0], rx_sem.at[rel, k], partner).wait_recv()
            remote(vt.at[rel, k], vt.at[rel, k], so_v.at[0, 0], rv_sem.at[rel, k], partner).wait_recv()
            pltpu.make_async_copy(xall.at[rel, k], xr.at[slot], ld_sem.at[slot]).start()

        @pl.when(jnp.logical_and(rel >= 2, lax.rem(rel, 2) == 0))
        def _():
            for copy in forward_partner(rel, k):
                copy.start()

        @pl.when(jnp.logical_and(rel == 2, lax.rem(k, 2) == 1))
        def _():
            for copy in forward_nbr(2, k, nbr_y):
                copy.start()

        @pl.when(jnp.logical_and(rel == 4, lax.rem(k, 2) == 0))
        def _():
            for copy in forward_nbr(4, k, nbr_x):
                copy.start()

    def trip(s, first):
        if first:
            fetch(jnp.int32(1))
        else:

            @pl.when(s + 1 < STEPS)
            def _():
                fetch(s + 1)

            done, number, _ = stream_of(s - 2)

            @pl.when(jnp.logical_and(done, s >= 2))
            def _():
                write_k(number).start()

        streamed, number, k_slot = stream_of(s)

        @pl.when(jnp.logical_and(streamed, number >= RING))
        def _():
            write_k(number - RING).wait()

        x_slot = lax.rem(s, XR)
        n_slot = lax.rem(s, 2)
        load_own(0, x_slot).wait()
        rel, k = chunk_of(s)
        for p in range(NP):
            rows = slice(p * PIECE, (p + 1) * PIECE)
            part = xr[x_slot, rows, :].astype(jnp.float32)
            norm = jnp.sum(part * part, axis=1, keepdims=True)
            nj[n_slot, rows, :] = jnp.broadcast_to(norm, (PIECE, T))
        for i in range(NCH):
            tile(x_slot, k_slot, n_slot, i)
            if i >= 1:
                apply(k_slot, vt[rel, k], i - 1)
        apply(k_slot, vt[rel, k], NCH - 1)

    trip(jnp.int32(0), True)

    @pl.loop(1, STEPS)
    def _(s):
        trip(s, False)

    @pl.loop(0, NCH)
    def _(k):
        yall[0, k] = ysum[k].astype(jnp.bfloat16)
        ysum[k] = jnp.zeros((COLS, T), jnp.float32)

    for back in (2, 1):
        streamed, number, _ = stream_of(jnp.int32(STEPS - back))

        @pl.when(streamed)
        def _():
            write_k(number).start()

    @pl.loop(0, NCH)
    def _(k):
        for which, dev in enumerate((partner, nbr_x, nbr_y)):
            for copy in send_own(k, which, dev):
                copy.wait_send()
        for rel in (2, 4, 6):
            for copy in forward_partner(rel, k):
                copy.wait_send()
        for copy in forward_nbr(2, k, nbr_y):
            copy.wait_send()

    half = NCH // 2

    def y_copy(src_rel, dst_rel, lo, n, idx, dev):
        return remote(
            yall.at[src_rel, pl.ds(lo, n)], yall.at[dst_rel, pl.ds(lo, n)], ys_sem.at[idx], yr_sem.at[idx], dev
        )

    y_moves = (
        (0, 1, 0, NCH, partner),
        (0, 2, 0, NCH, nbr_x),
        (0, 4, 0, NCH, nbr_y),
        (2, 3, 0, NCH, partner),
        (4, 5, 0, NCH, partner),
        (4, 6, 0, half, nbr_x),
        (2, 6, half, half, nbr_y),
        (6, 7, 0, NCH, partner),
    )

    def y_move(idx):
        src, dst, lo, n, dev = y_moves[idx]
        return y_copy(src, dst, lo, n, idx, dev)

    def y_arrived(idx):
        _, dst, lo, n, dev = y_moves[idx]
        return y_copy(dst, dst, lo, n, idx, dev)

    for idx in range(3):
        y_move(idx).start()

    for back in range(RING):
        write_k(jnp.int32(N_STREAM - RING + back)).wait()
    for number in range(RING):
        read_k(jnp.int32(number)).start()

    def second(s):
        @pl.when(s == 12)
        def _():
            y_arrived(0).wait_recv()

        @pl.when(s == 20)
        def _():
            y_arrived(1).wait_recv()
            y_arrived(2).wait_recv()
            for idx in range(3, 7):
                y_move(idx).start()

        @pl.when(s == 28)
        def _():
            y_arrived(3).wait_recv()
            y_arrived(4).wait_recv()

        @pl.when(s == 56)
        def _():
            y_arrived(5).wait_recv()
            y_arrived(6).wait_recv()
            y_move(7).start()

        @pl.when(s == 70)
        def _():
            y_arrived(7).wait_recv()

        streamed, number, slot = stream_of(s)

        @pl.when(streamed)
        def _():
            read_k(number).wait()

        rel, k = chunk_of(s)
        for i in range(NCH):
            apply(slot, yall[rel, k], i)

        @pl.when(jnp.logical_and(streamed, number + RING < N_STREAM))
        def _():
            read_k(number + RING).start()

    @pl.loop(0, STEPS)
    def _(s):
        second(s)

    for idx in range(8):
        y_move(idx).wait_send()

    @pl.loop(0, NCH)
    def _(k):
        out_ref[k] = ysum[k]


def solution(mesh):
    rows = NCH * T

    def local_program(x_loc, v_loc, length_scale, out_scale):
        vt_loc = v_loc.reshape(NCH, T, COLS).transpose(0, 2, 1)
        dma = pltpu.SemaphoreType.DMA
        out, _, _ = pl.pallas_call(
            body,
            out_shape=(
                jax.ShapeDtypeStruct((NCH, COLS, T), jnp.float32),
                jax.ShapeDtypeStruct((NREL, NCH, T, FEAT), jnp.bfloat16),
                jax.ShapeDtypeStruct((N_STREAM, NCH, T, T), jnp.bfloat16),
            ),
            in_specs=[
                pl.BlockSpec(memory_space=pltpu.HBM),
                pl.BlockSpec(memory_space=pltpu.HBM),
                pl.BlockSpec(memory_space=pltpu.SMEM),
                pl.BlockSpec(memory_space=pltpu.SMEM),
            ],
            out_specs=(
                pl.BlockSpec(memory_space=pltpu.VMEM),
                pl.BlockSpec(memory_space=pltpu.HBM),
                pl.BlockSpec(memory_space=pltpu.HBM),
            ),
            scratch_shapes=[
                pltpu.VMEM((NCH, FEAT, T), jnp.bfloat16),
                pltpu.VMEM((NREL, NCH, COLS, T), jnp.bfloat16),
                pltpu.VMEM((NREL, NCH, COLS, T), jnp.bfloat16),
                pltpu.VMEM((N_RES + RING, NCH, T, T), jnp.bfloat16),
                pltpu.VMEM((XR, T, FEAT), jnp.bfloat16),
                pltpu.VMEM((2, T, T), jnp.float32),
                pltpu.VMEM((NCH, 8, T), jnp.float32),
                dma((XR,)), dma((RING,)), dma((RING,)), dma,
                dma((NREL, NCH)), dma((NREL, NCH)),
                dma((3, NCH)), dma((3, NCH)),
                dma((3, NCH)), dma((3, NCH)),
                dma((NCH,)), dma((NCH,)),
                dma((8,)), dma((8,)),
                pltpu.VMEM((NCH, COLS, T), jnp.float32),
            ],
            compiler_params=pltpu.CompilerParams(
                collective_id=0, has_side_effects=True, vmem_limit_bytes=67_043_328
            ),
        )(x_loc.reshape(NCH, T, FEAT), vt_loc, length_scale, out_scale)
        return out.transpose(0, 2, 1).reshape(rows, COLS)

    row_spec = P(("task", "row"), None)
    return jax.shard_map(
        local_program,
        mesh=mesh,
        in_specs=(row_spec, row_spec, P("task"), P("task")),
        out_specs=row_spec,
        check_vma=False,
    )
```

```python
import functools
import math

import jax
import jax.numpy as jnp
from jax import lax
from jax.experimental import pallas as pl
from jax.experimental.pallas import tpu as pltpu
from jax.sharding import PartitionSpec as P

MESH = pl.DeviceIdType.MESH
T = 256
FEAT = 512
COLS = 64
NCH = 12
NREL = 8
STEPS = NREL * NCH
PIECE = 64
NP = T // PIECE
NI = NCH // 2
RES_IN, RES_OF = 3, 8
N_RES = (STEPS - 24) // RES_OF * RES_IN
RING = 5
N_STREAM = STEPS - N_RES
XR = 3


def chunk_of(s):
    j = lax.rem(s + 2, 4)
    v = lax.div(s - 22, 4) - 1
    late = jnp.where(s < 26, 0, jnp.where(s >= 94, 1, lax.div(j, 2)))
    group = jnp.where(s < 26, 0, jnp.where(s >= 94, 17, v + 1 - late))
    side = lax.rem(s, 2)
    far = group >= 12
    rel = jnp.where(far, 6, 2 + 2 * side) + late
    chunk = jnp.where(far, 2 * (group - 12) + side, group)
    near_rel = lax.div(s, NCH)
    near_chunk = lax.rem(s, NCH)
    return jnp.where(s < 24, near_rel, rel), jnp.where(s < 24, near_chunk, chunk)


def stream_of(s):
    u = jnp.maximum(s - 24, 0)
    w = lax.rem(u, RES_OF)
    o = lax.div(u, RES_OF)
    streamed = jnp.logical_or(s < 24, w >= RES_IN)
    number = jnp.where(s < 24, s, 24 + o * (RES_OF - RES_IN) + w - RES_IN)
    slot = jnp.where(streamed, N_RES + lax.rem(number, RING), o * RES_IN + w)
    return streamed, number, slot


def body(
    x_hbm, vt_hbm, ls_ref, os_ref,
    out_ref, xall, kst,
    xt, vt, yall, kbuf, xr, nj, ni,
    ld_sem, kw_sem, kr_sem, vl_sem,
    rx_sem, rv_sem, so_x, so_v, sp_x, sp_v, sn_x, sn_v, ys_sem, yr_sem,
    ysum,
):
    me = lax.axis_index("row")
    partner = me + 1 - 2 * lax.rem(me, 2)
    nbr_x = me + 2 - 4 * lax.rem(lax.div(me, 2), 2)
    nbr_y = me + 4 - 8 * lax.div(me, 4)

    def remote(src, dst, ss, rs, dev):
        return pltpu.make_async_remote_copy(
            src_ref=src, dst_ref=dst, send_sem=ss, recv_sem=rs, device_id={"row": dev}, device_id_type=MESH
        )

    def send_own(k, which, dev):
        slot = (1, 2, 4)[which]
        return (
            remote(x_hbm.at[k], xall.at[slot, k], so_x.at[which, k], rx_sem.at[slot, k], dev),
            remote(vt_hbm.at[k], vt.at[slot, k], so_v.at[which, k], rv_sem.at[slot, k], dev),
        )

    def forward_partner(rel, k):
        row = lax.div(rel, 2) - 1
        return (
            remote(xall.at[rel, k], xall.at[rel + 1, k], sp_x.at[row, k], rx_sem.at[rel + 1, k], partner),
            remote(vt.at[rel, k], vt.at[rel + 1, k], sp_v.at[row, k], rv_sem.at[rel + 1, k], partner),
        )

    def forward_nbr(rel, k, dev):
        return (
            remote(xall.at[rel, k], xall.at[6, k], sn_x.at[k], rx_sem.at[6, k], dev),
            remote(vt.at[rel, k], vt.at[6, k], sn_v.at[k], rv_sem.at[6, k], dev),
        )

    barrier = pltpu.get_barrier_semaphore()
    for dev in (partner, nbr_x, nbr_y):
        pl.semaphore_signal(barrier, inc=1, device_id={"row": dev}, device_id_type=MESH)

    own_v = pltpu.make_async_copy(vt_hbm, vt.at[0], vl_sem)
    own_v.start()

    def load_own(k, slot):
        return pltpu.make_async_copy(x_hbm.at[k], xr.at[slot], ld_sem.at[slot])

    load_own(0, 0).start()
    pl.semaphore_wait(barrier, 3)

    @pl.loop(0, NCH)
    def _(k):
        for which, dev in enumerate((partner, nbr_x, nbr_y)):
            for copy in send_own(k, which, dev):
                copy.start()

    load_own(1, 1).start()

    @pl.loop(0, NCH)
    def _(k):
        slot = lax.rem(k, 2)
        load_own(k, slot).wait()
        norm = jnp.zeros((1, T), jnp.float32)
        for h in range(2):
            part = xr[slot, :, h * T : (h + 1) * T].astype(jnp.float32).T
            norm = norm + jnp.sum(part * part, axis=0, keepdims=True)
            xt[k, h * T : (h + 1) * T, :] = (part * -2.0).astype(jnp.bfloat16)
        ni[k] = jnp.broadcast_to(norm, (8, T))

        @pl.when(k + 2 < NCH)
        def _():
            load_own(k + 2, slot).start()

    own_v.wait()
    load_own(0, 0).start()

    scale = jnp.full((1, T), ls_ref[0], jnp.float32)
    rate = -math.log2(math.e) / (2.0 * scale * scale)
    amp = jnp.full((1, T), os_ref[0], jnp.float32)

    @pl.loop(0, NCH)
    def _(k):
        ysum[k] = jnp.zeros((COLS, T), jnp.float32)

    def write_k(number):
        slot = lax.rem(number, RING)
        return pltpu.make_async_copy(kbuf.at[N_RES + slot], kst.at[number], kw_sem.at[slot])

    def read_k(number):
        slot = lax.rem(number, RING)
        return pltpu.make_async_copy(kst.at[number], kbuf.at[N_RES + slot], kr_sem.at[slot])

    def gram(x_slot, i):
        return jnp.dot(xr[x_slot], xt[i], preferred_element_type=jnp.float32)

    def weigh(gram_tile, k_slot, n_slot, i):
        dist = jnp.maximum((nj[n_slot] + ni[i, 0:1, :]) + gram_tile, 0.0)
        kbuf[k_slot, i] = (amp * jnp.exp2(dist * rate)).astype(jnp.bfloat16)

    def apply(k_slot, lhs, i):
        ysum[i] += jnp.dot(lhs, kbuf[k_slot, i], preferred_element_type=jnp.float32)

    def fetch(s):
        rel, k = chunk_of(s)
        slot = lax.rem(s, XR)

        @pl.when(rel == 0)
        def _():
            load_own(k, slot).start()

        @pl.when(rel > 0)
        def _():
            remote(xall.at[rel, k], xall.at[rel, k], so_x.at[0, 0], rx_sem.at[rel, k], partner).wait_recv()
            remote(vt.at[rel, k], vt.at[rel, k], so_v.at[0, 0], rv_sem.at[rel, k], partner).wait_recv()
            pltpu.make_async_copy(xall.at[rel, k], xr.at[slot], ld_sem.at[slot]).start()

        @pl.when(jnp.logical_and(rel >= 2, lax.rem(rel, 2) == 0))
        def _():
            for copy in forward_partner(rel, k):
                copy.start()

        @pl.when(jnp.logical_and(rel == 2, lax.rem(k, 2) == 1))
        def _():
            for copy in forward_nbr(2, k, nbr_y):
                copy.start()

        @pl.when(jnp.logical_and(rel == 4, lax.rem(k, 2) == 0))
        def _():
            for copy in forward_nbr(4, k, nbr_x):
                copy.start()

    def trip(s, first):
        if first:
            fetch(jnp.int32(1))
        else:

            @pl.when(s + 1 < STEPS)
            def _():
                fetch(s + 1)

            done, number, _ = stream_of(s - 2)

            @pl.when(jnp.logical_and(done, s >= 2))
            def _():
                write_k(number).start()

        streamed, number, k_slot = stream_of(s)

        @pl.when(jnp.logical_and(streamed, number >= RING))
        def _():
            write_k(number - RING).wait()

        x_slot = lax.rem(s, XR)
        n_slot = lax.rem(s, 2)
        load_own(0, x_slot).wait()
        rel, k = chunk_of(s)
        for p in range(NP):
            rows = slice(p * PIECE, (p + 1) * PIECE)
            part = xr[x_slot, rows, :].astype(jnp.float32)
            norm = jnp.sum(part * part, axis=1, keepdims=True)
            nj[n_slot, rows, :] = jnp.broadcast_to(norm, (PIECE, T))
        for i in range(NCH):
            weigh(gram(x_slot, i), k_slot, n_slot, i)
        for i in range(NCH):
            apply(k_slot, vt[rel, k], i)

    trip(jnp.int32(0), True)

    @pl.loop(1, STEPS)
    def _(s):
        trip(s, False)

    @pl.loop(0, NCH)
    def _(k):
        yall[0, k] = ysum[k].astype(jnp.bfloat16)
        ysum[k] = jnp.zeros((COLS, T), jnp.float32)

    for back in (2, 1):
        streamed, number, _ = stream_of(jnp.int32(STEPS - back))

        @pl.when(streamed)
        def _():
            write_k(number).start()

    @pl.loop(0, NCH)
    def _(k):
        for which, dev in enumerate((partner, nbr_x, nbr_y)):
            for copy in send_own(k, which, dev):
                copy.wait_send()
        for rel in (2, 4, 6):
            for copy in forward_partner(rel, k):
                copy.wait_send()
        for copy in forward_nbr(2, k, nbr_y):
            copy.wait_send()

    half = NCH // 2

    def y_copy(src_rel, dst_rel, lo, n, idx, dev):
        return remote(
            yall.at[src_rel, pl.ds(lo, n)], yall.at[dst_rel, pl.ds(lo, n)], ys_sem.at[idx], yr_sem.at[idx], dev
        )

    y_moves = (
        (0, 1, 0, NCH, partner),
        (0, 2, 0, NCH, nbr_x),
        (0, 4, 0, NCH, nbr_y),
        (2, 3, 0, NCH, partner),
        (4, 5, 0, NCH, partner),
        (4, 6, 0, half, nbr_x),
        (2, 6, half, half, nbr_y),
        (6, 7, 0, NCH, partner),
    )

    def y_move(idx):
        src, dst, lo, n, dev = y_moves[idx]
        return y_copy(src, dst, lo, n, idx, dev)

    def y_arrived(idx):
        _, dst, lo, n, dev = y_moves[idx]
        return y_copy(dst, dst, lo, n, idx, dev)

    for idx in range(3):
        y_move(idx).start()

    for back in range(RING):
        write_k(jnp.int32(N_STREAM - RING + back)).wait()
    for number in range(RING):
        read_k(jnp.int32(number)).start()

    def second(s):
        @pl.when(s == 12)
        def _():
            y_arrived(0).wait_recv()

        @pl.when(s == 20)
        def _():
            y_arrived(1).wait_recv()
            y_arrived(2).wait_recv()
            for idx in range(3, 7):
                y_move(idx).start()

        @pl.when(s == 28)
        def _():
            y_arrived(3).wait_recv()
            y_arrived(4).wait_recv()

        @pl.when(s == 56)
        def _():
            y_arrived(5).wait_recv()
            y_arrived(6).wait_recv()
            y_move(7).start()

        @pl.when(s == 70)
        def _():
            y_arrived(7).wait_recv()

        streamed, number, slot = stream_of(s)

        @pl.when(streamed)
        def _():
            read_k(number).wait()

        rel, k = chunk_of(s)
        for i in range(NCH):
            apply(slot, yall[rel, k], i)

        @pl.when(jnp.logical_and(streamed, number + RING < N_STREAM))
        def _():
            read_k(number + RING).start()

    @pl.loop(0, STEPS)
    def _(s):
        second(s)

    for idx in range(8):
        y_move(idx).wait_send()

    @pl.loop(0, NCH)
    def _(k):
        out_ref[k] = ysum[k]


def solution(mesh):
    rows = NCH * T

    def local_program(x_loc, v_loc, length_scale, out_scale):
        vt_loc = v_loc.reshape(NCH, T, COLS).transpose(0, 2, 1)
        dma = pltpu.SemaphoreType.DMA
        out, _, _ = pl.pallas_call(
            body,
            out_shape=(
                jax.ShapeDtypeStruct((NCH, COLS, T), jnp.float32),
                jax.ShapeDtypeStruct((NREL, NCH, T, FEAT), jnp.bfloat16),
                jax.ShapeDtypeStruct((N_STREAM, NCH, T, T), jnp.bfloat16),
            ),
            in_specs=[
                pl.BlockSpec(memory_space=pltpu.HBM),
                pl.BlockSpec(memory_space=pltpu.HBM),
                pl.BlockSpec(memory_space=pltpu.SMEM),
                pl.BlockSpec(memory_space=pltpu.SMEM),
            ],
            out_specs=(
                pl.BlockSpec(memory_space=pltpu.VMEM),
                pl.BlockSpec(memory_space=pltpu.HBM),
                pl.BlockSpec(memory_space=pltpu.HBM),
            ),
            scratch_shapes=[
                pltpu.VMEM((NCH, FEAT, T), jnp.bfloat16),
                pltpu.VMEM((NREL, NCH, COLS, T), jnp.bfloat16),
                pltpu.VMEM((NREL, NCH, COLS, T), jnp.bfloat16),
                pltpu.VMEM((N_RES + RING, NCH, T, T), jnp.bfloat16),
                pltpu.VMEM((XR, T, FEAT), jnp.bfloat16),
                pltpu.VMEM((2, T, T), jnp.float32),
                pltpu.VMEM((NCH, 8, T), jnp.float32),
                dma((XR,)), dma((RING,)), dma((RING,)), dma,
                dma((NREL, NCH)), dma((NREL, NCH)),
                dma((3, NCH)), dma((3, NCH)),
                dma((3, NCH)), dma((3, NCH)),
                dma((NCH,)), dma((NCH,)),
                dma((8,)), dma((8,)),
                pltpu.VMEM((NCH, COLS, T), jnp.float32),
            ],
            compiler_params=pltpu.CompilerParams(
                collective_id=0, has_side_effects=True, vmem_limit_bytes=67_043_328
            ),
        )(x_loc.reshape(NCH, T, FEAT), vt_loc, length_scale, out_scale)
        return out.transpose(0, 2, 1).reshape(rows, COLS)

    row_spec = P(("task", "row"), None)
    return jax.shard_map(
        local_program,
        mesh=mesh,
        in_specs=(row_spec, row_spec, P("task"), P("task")),
        out_specs=row_spec,
        check_vma=False,
    )
```

```python
import functools
import math

import jax
import jax.numpy as jnp
from jax import lax
from jax.experimental import pallas as pl
from jax.experimental.pallas import tpu as pltpu
from jax.sharding import PartitionSpec as P

MESH = pl.DeviceIdType.MESH
T = 256
FEAT = 512
COLS = 64
NCH = 12
NREL = 8
STEPS = NREL * NCH
PIECE = 64
NP = T // PIECE
NI = NCH // 2
PAIRS = STEPS // 2
RES_IN, RES_OF = 2, 5
N_RES = (PAIRS - 12) // RES_OF * RES_IN
RING = 3
N_STREAM = PAIRS - N_RES
XR = 2


def chunk_of(s):
    j = lax.rem(s + 2, 4)
    v = lax.div(s - 22, 4) - 1
    late = jnp.where(s < 26, 0, jnp.where(s >= 94, 1, lax.div(j, 2)))
    group = jnp.where(s < 26, 0, jnp.where(s >= 94, 17, v + 1 - late))
    side = lax.rem(s, 2)
    far = group >= 12
    rel = jnp.where(far, 6, 2 + 2 * side) + late
    chunk = jnp.where(far, 2 * (group - 12) + side, group)
    near_rel = lax.div(s, NCH)
    near_chunk = lax.rem(s, NCH)
    return jnp.where(s < 24, near_rel, rel), jnp.where(s < 24, near_chunk, chunk)


def stream_of(t):
    u = jnp.maximum(t - 12, 0)
    w = lax.rem(u, RES_OF)
    o = lax.div(u, RES_OF)
    keep = jnp.where(o == (PAIRS - 12) // RES_OF, 0, RES_IN)
    streamed = jnp.logical_or(t < 12, w >= keep)
    number = jnp.where(t < 12, t, 12 + o * (RES_OF - RES_IN) + w - keep)
    return streamed, number, o * RES_IN + w


def body(
    x_hbm, vt_hbm, ls_ref, os_ref,
    out_ref, xall, kst,
    xt, vt, yall, kept, stage, xr, nj, ni,
    ld_sem, kw_sem, kr_sem, vl_sem,
    rx_sem, rv_sem, so_x, so_v, sp_x, sp_v, sn_x, sn_v, ys_sem, yr_sem,
    ysum,
):
    me = lax.axis_index("row")
    partner = me + 1 - 2 * lax.rem(me, 2)
    nbr_x = me + 2 - 4 * lax.rem(lax.div(me, 2), 2)
    nbr_y = me + 4 - 8 * lax.div(me, 4)

    def remote(src, dst, ss, rs, dev):
        return pltpu.make_async_remote_copy(
            src_ref=src, dst_ref=dst, send_sem=ss, recv_sem=rs, device_id={"row": dev}, device_id_type=MESH
        )

    def send_own(k, which, dev):
        slot = (1, 2, 4)[which]
        return (
            remote(x_hbm.at[k], xall.at[slot, k], so_x.at[which, k], rx_sem.at[slot, k], dev),
            remote(vt_hbm.at[k], vt.at[slot, k], so_v.at[which, k], rv_sem.at[slot, k], dev),
        )

    def forward_partner(rel, k):
        row = lax.div(rel, 2) - 1
        return (
            remote(xall.at[rel, k], xall.at[rel + 1, k], sp_x.at[row, k], rx_sem.at[rel + 1, k], partner),
            remote(vt.at[rel, k], vt.at[rel + 1, k], sp_v.at[row, k], rv_sem.at[rel + 1, k], partner),
        )

    def forward_nbr(rel, k, dev):
        return (
            remote(xall.at[rel, k], xall.at[6, k], sn_x.at[k], rx_sem.at[6, k], dev),
            remote(vt.at[rel, k], vt.at[6, k], sn_v.at[k], rv_sem.at[6, k], dev),
        )

    barrier = pltpu.get_barrier_semaphore()
    for dev in (partner, nbr_x, nbr_y):
        pl.semaphore_signal(barrier, inc=1, device_id={"row": dev}, device_id_type=MESH)

    own_v = pltpu.make_async_copy(vt_hbm, vt.at[0], vl_sem)
    own_v.start()

    def load_own(k, slot, half):
        return pltpu.make_async_copy(x_hbm.at[k], xr.at[slot, pl.ds(half * T, T)], ld_sem.at[slot, half])

    load_own(0, 0, 0).start()
    pl.semaphore_wait(barrier, 3)

    @pl.loop(0, NCH)
    def _(k):
        for which, dev in enumerate((partner, nbr_x, nbr_y)):
            for copy in send_own(k, which, dev):
                copy.start()

    load_own(1, 1, 0).start()

    @pl.loop(0, NCH)
    def _(k):
        slot = lax.rem(k, 2)
        load_own(k, slot, 0).wait()
        norm = jnp.zeros((1, T), jnp.float32)
        for h in range(2):
            part = xr[slot, :T, h * T : (h + 1) * T].astype(jnp.float32).T
            norm = norm + jnp.sum(part * part, axis=0, keepdims=True)
            xt[k, h * T : (h + 1) * T, :] = (part * -2.0).astype(jnp.bfloat16)
        ni[k] = jnp.broadcast_to(norm, (8, T))

        @pl.when(k + 2 < NCH)
        def _():
            load_own(k + 2, slot, 0).start()

    own_v.wait()
    load_own(0, 0, 0).start()
    load_own(1, 0, 1).start()

    scale = jnp.full((1, 128), ls_ref[0], jnp.float32)
    rate = -math.log2(math.e) / (2.0 * scale * scale)
    amp = jnp.full((1, 128), os_ref[0], jnp.float32)

    @pl.loop(0, NCH)
    def _(k):
        ysum[k] = jnp.zeros((COLS, T), jnp.float32)

    def write_k(t, parity):
        streamed, number, slot = stream_of(t)

        @pl.when(streamed)
        def _():
            pltpu.make_async_copy(stage.at[parity], kst.at[number], kw_sem.at[parity]).start()

        @pl.when(jnp.logical_not(streamed))
        def _():
            pltpu.make_async_copy(stage.at[parity], kept.at[slot], kw_sem.at[parity]).start()

    def written(parity):
        pltpu.make_async_copy(stage.at[parity], kst.at[0], kw_sem.at[parity]).wait()

    def read_k(number):
        slot = lax.rem(number, RING)
        return pltpu.make_async_copy(kst.at[number], stage.at[slot], kr_sem.at[slot])

    def weigh(x_slot, parity, i):
        gram_tile = jnp.dot(xr[x_slot], xt[i], preferred_element_type=jnp.float32)
        for h in range(2):
            lanes = slice(h * 128, (h + 1) * 128)
            dist = jnp.maximum((nj[...] + ni[i, 0:1, lanes]) + gram_tile[:, lanes], 0.0)
            stage[parity, i, :, lanes] = (amp * jnp.exp2(dist * rate)).astype(jnp.bfloat16)

    def apply(source, slot, lhs, i):
        ysum[i] += jnp.dot(lhs, source[slot, i], preferred_element_type=jnp.float32)

    def pair_of(table, t):
        rel, k = chunk_of(2 * t)
        rel_2, k_2 = chunk_of(2 * t + 1)
        return jnp.concatenate([table[rel, k], table[rel_2, k_2]], axis=1)

    def fetch(s):
        rel, k = chunk_of(s)
        half = lax.rem(s, 2)
        slot = lax.rem(lax.div(s, 2), XR)

        @pl.when(rel == 0)
        def _():
            load_own(k, slot, half).start()

        @pl.when(rel > 0)
        def _():
            remote(xall.at[rel, k], xall.at[rel, k], so_x.at[0, 0], rx_sem.at[rel, k], partner).wait_recv()
            remote(vt.at[rel, k], vt.at[rel, k], so_v.at[0, 0], rv_sem.at[rel, k], partner).wait_recv()
            pltpu.make_async_copy(
                xall.at[rel, k], xr.at[slot, pl.ds(half * T, T)], ld_sem.at[slot, half]
            ).start()

        @pl.when(jnp.logical_and(rel >= 2, lax.rem(rel, 2) == 0))
        def _():
            for copy in forward_partner(rel, k):
                copy.start()

        @pl.when(jnp.logical_and(rel == 2, lax.rem(k, 2) == 1))
        def _():
            for copy in forward_nbr(2, k, nbr_y):
                copy.start()

        @pl.when(jnp.logical_and(rel == 4, lax.rem(k, 2) == 0))
        def _():
            for copy in forward_nbr(4, k, nbr_x):
                copy.start()

    def trip(t, parity, place):
        if place < 2:
            fetch(2 * t + 2)
            fetch(2 * t + 3)
        if place > 0:
            write_k(t - 1, 1 - parity)

            @pl.when(t >= 2)
            def _():
                written(parity)

        x_slot = parity
        load_own(0, x_slot, 0).wait()
        load_own(0, x_slot, 1).wait()
        for p in range(2 * NP):
            rows = slice(p * PIECE, (p + 1) * PIECE)
            part = xr[x_slot, rows, :].astype(jnp.float32)
            norm = jnp.sum(part * part, axis=1, keepdims=True)
            nj[rows, :] = jnp.broadcast_to(norm, (PIECE, 128))
        if place > 0:
            lhs = pair_of(vt, t - 1)
        for i in range(NCH):
            if place > 0:
                apply(stage, 1 - parity, lhs, i)
            weigh(x_slot, parity, i)

    trip(jnp.int32(0), 0, 0)

    @pl.loop(0, PAIRS // 2 - 1)
    def _(m):
        trip(2 * m + 1, 1, 1)
        trip(2 * m + 2, 0, 1)

    trip(jnp.int32(PAIRS - 1), 1, 2)
    write_k(jnp.int32(PAIRS - 1), 1)
    lhs = pair_of(vt, jnp.int32(PAIRS - 1))
    for i in range(NCH):
        apply(stage, 1, lhs, i)

    @pl.loop(0, NCH)
    def _(k):
        yall[0, k] = ysum[k].astype(jnp.bfloat16)
        ysum[k] = jnp.zeros((COLS, T), jnp.float32)

    @pl.loop(0, NCH)
    def _(k):
        for which, dev in enumerate((partner, nbr_x, nbr_y)):
            for copy in send_own(k, which, dev):
                copy.wait_send()
        for rel in (2, 4, 6):
            for copy in forward_partner(rel, k):
                copy.wait_send()
        for copy in forward_nbr(2, k, nbr_y):
            copy.wait_send()

    half = NCH // 2

    def y_copy(src_rel, dst_rel, lo, n, idx, dev):
        return remote(
            yall.at[src_rel, pl.ds(lo, n)], yall.at[dst_rel, pl.ds(lo, n)], ys_sem.at[idx], yr_sem.at[idx], dev
        )

    y_moves = (
        (0, 1, 0, NCH, partner),
        (0, 2, 0, NCH, nbr_x),
        (0, 4, 0, NCH, nbr_y),
        (2, 3, 0, NCH, partner),
        (4, 5, 0, NCH, partner),
        (4, 6, 0, half, nbr_x),
        (2, 6, half, half, nbr_y),
        (6, 7, 0, NCH, partner),
    )

    def y_move(idx):
        src, dst, lo, n, dev = y_moves[idx]
        return y_copy(src, dst, lo, n, idx, dev)

    def y_arrived(idx):
        _, dst, lo, n, dev = y_moves[idx]
        return y_copy(dst, dst, lo, n, idx, dev)

    for idx in range(3):
        y_move(idx).start()

    for parity in range(2):
        written(parity)
    for number in range(RING):
        read_k(jnp.int32(number)).start()

    def second(t):
        s = 2 * t

        @pl.when(s == 12)
        def _():
            y_arrived(0).wait_recv()

        @pl.when(s == 20)
        def _():
            y_arrived(1).wait_recv()
            y_arrived(2).wait_recv()
            for idx in range(3, 7):
                y_move(idx).start()

        @pl.when(s == 28)
        def _():
            y_arrived(3).wait_recv()
            y_arrived(4).wait_recv()

        @pl.when(s == 56)
        def _():
            y_arrived(5).wait_recv()
            y_arrived(6).wait_recv()
            y_move(7).start()

        @pl.when(s == 70)
        def _():
            y_arrived(7).wait_recv()

        streamed, number, slot = stream_of(t)

        @pl.when(streamed)
        def _():
            read_k(number).wait()

        lhs = pair_of(yall, t)

        @pl.when(streamed)
        def _():
            for i in range(NCH):
                apply(stage, lax.rem(number, RING), lhs, i)

        @pl.when(jnp.logical_not(streamed))
        def _():
            for i in range(NCH):
                apply(kept, slot, lhs, i)

        @pl.when(jnp.logical_and(streamed, number + RING < N_STREAM))
        def _():
            read_k(number + RING).start()

    @pl.loop(0, PAIRS)
    def _(t):
        second(t)

    for idx in range(8):
        y_move(idx).wait_send()

    @pl.loop(0, NCH)
    def _(k):
        out_ref[k] = ysum[k]


def solution(mesh):
    rows = NCH * T

    def local_program(x_loc, v_loc, length_scale, out_scale):
        vt_loc = v_loc.reshape(NCH, T, COLS).transpose(0, 2, 1)
        dma = pltpu.SemaphoreType.DMA
        out, _, _ = pl.pallas_call(
            body,
            out_shape=(
                jax.ShapeDtypeStruct((NCH, COLS, T), jnp.float32),
                jax.ShapeDtypeStruct((NREL, NCH, T, FEAT), jnp.bfloat16),
                jax.ShapeDtypeStruct((N_STREAM, NCH, 2 * T, T), jnp.bfloat16),
            ),
            in_specs=[
                pl.BlockSpec(memory_space=pltpu.HBM),
                pl.BlockSpec(memory_space=pltpu.HBM),
                pl.BlockSpec(memory_space=pltpu.SMEM),
                pl.BlockSpec(memory_space=pltpu.SMEM),
            ],
            out_specs=(
                pl.BlockSpec(memory_space=pltpu.VMEM),
                pl.BlockSpec(memory_space=pltpu.HBM),
                pl.BlockSpec(memory_space=pltpu.HBM),
            ),
            scratch_shapes=[
                pltpu.VMEM((NCH, FEAT, T), jnp.bfloat16),
                pltpu.VMEM((NREL, NCH, COLS, T), jnp.bfloat16),
                pltpu.VMEM((NREL, NCH, COLS, T), jnp.bfloat16),
                pltpu.VMEM((N_RES, NCH, 2 * T, T), jnp.bfloat16),
                pltpu.VMEM((RING, NCH, 2 * T, T), jnp.bfloat16),
                pltpu.VMEM((XR, 2 * T, FEAT), jnp.bfloat16),
                pltpu.VMEM((2 * T, 128), jnp.float32),
                pltpu.VMEM((NCH, 8, T), jnp.float32),
                dma((XR, 2)), dma((2,)), dma((RING,)), dma,
                dma((NREL, NCH)), dma((NREL, NCH)),
                dma((3, NCH)), dma((3, NCH)),
                dma((3, NCH)), dma((3, NCH)),
                dma((NCH,)), dma((NCH,)),
                dma((8,)), dma((8,)),
                pltpu.VMEM((NCH, COLS, T), jnp.float32),
            ],
            compiler_params=pltpu.CompilerParams(
                collective_id=0, has_side_effects=True, vmem_limit_bytes=67_043_328
            ),
        )(x_loc.reshape(NCH, T, FEAT), vt_loc, length_scale, out_scale)
        return out.transpose(0, 2, 1).reshape(rows, COLS)

    row_spec = P(("task", "row"), None)
    return jax.shard_map(
        local_program,
        mesh=mesh,
        in_specs=(row_spec, row_spec, P("task"), P("task")),
        out_specs=row_spec,
        check_vma=False,
    )
```

```python
import functools
import math

import jax
import jax.numpy as jnp
from jax import lax
from jax.experimental import pallas as pl
from jax.experimental.pallas import tpu as pltpu
from jax.sharding import PartitionSpec as P

MESH = pl.DeviceIdType.MESH
T = 256
FEAT = 512
COLS = 64
NCH = 12
NREL = 8
STEPS = NREL * NCH
PIECE = 64
NP = T // PIECE
NI = NCH // 2
PAIRS = STEPS // 2
RES_IN, RES_OF = 2, 5
N_RES = (PAIRS - 12) // RES_OF * RES_IN
RING = 3
N_STREAM = PAIRS - N_RES
XR = 2


def chunk_of(s):
    j = lax.rem(s + 2, 4)
    v = lax.div(s - 22, 4) - 1
    late = jnp.where(s < 26, 0, jnp.where(s >= 94, 1, lax.div(j, 2)))
    group = jnp.where(s < 26, 0, jnp.where(s >= 94, 17, v + 1 - late))
    side = lax.rem(s, 2)
    far = group >= 12
    rel = jnp.where(far, 6, 2 + 2 * side) + late
    chunk = jnp.where(far, 2 * (group - 12) + side, group)
    near_rel = lax.div(s, NCH)
    near_chunk = lax.rem(s, NCH)
    return jnp.where(s < 24, near_rel, rel), jnp.where(s < 24, near_chunk, chunk)


def wide(left, right):
    return jnp.concatenate([left, right], axis=1)


def stream_of(t):
    u = jnp.maximum(t - 12, 0)
    w = lax.rem(u, RES_OF)
    o = lax.div(u, RES_OF)
    keep = jnp.where(o == (PAIRS - 12) // RES_OF, 0, RES_IN)
    streamed = jnp.logical_or(t < 12, w >= keep)
    number = jnp.where(t < 12, t, 12 + o * (RES_OF - RES_IN) + w - keep)
    return streamed, number, o * RES_IN + w


def body(
    x_hbm, vt_hbm, ls_ref, os_ref,
    out_ref, xall, kst,
    xt, vt, yall, kept, stage, xr, nj, ni,
    ld_sem, kw_sem, kr_sem, vl_sem,
    rx_sem, rv_sem, so_x, so_v, sp_x, sp_v, sn_x, sn_v, ys_sem, yr_sem,
    ysum,
):
    me = lax.axis_index("row")
    partner = me + 1 - 2 * lax.rem(me, 2)
    nbr_x = me + 2 - 4 * lax.rem(lax.div(me, 2), 2)
    nbr_y = me + 4 - 8 * lax.div(me, 4)

    def remote(src, dst, ss, rs, dev):
        return pltpu.make_async_remote_copy(
            src_ref=src, dst_ref=dst, send_sem=ss, recv_sem=rs, device_id={"row": dev}, device_id_type=MESH
        )

    def send_own(k, which, dev):
        slot = (1, 2, 4)[which]
        return (
            remote(x_hbm.at[k], xall.at[slot, k], so_x.at[which, k], rx_sem.at[slot, k], dev),
            remote(vt_hbm.at[k], vt.at[slot, k], so_v.at[which, k], rv_sem.at[slot, k], dev),
        )

    def forward_partner(rel, k):
        row = lax.div(rel, 2) - 1
        return (
            remote(xall.at[rel, k], xall.at[rel + 1, k], sp_x.at[row, k], rx_sem.at[rel + 1, k], partner),
            remote(vt.at[rel, k], vt.at[rel + 1, k], sp_v.at[row, k], rv_sem.at[rel + 1, k], partner),
        )

    def forward_nbr(rel, k, dev):
        return (
            remote(xall.at[rel, k], xall.at[6, k], sn_x.at[k], rx_sem.at[6, k], dev),
            remote(vt.at[rel, k], vt.at[6, k], sn_v.at[k], rv_sem.at[6, k], dev),
        )

    barrier = pltpu.get_barrier_semaphore()
    for dev in (partner, nbr_x, nbr_y):
        pl.semaphore_signal(barrier, inc=1, device_id={"row": dev}, device_id_type=MESH)

    own_v = pltpu.make_async_copy(vt_hbm, vt.at[0], vl_sem)
    own_v.start()

    def load_own(k, slot, half):
        return pltpu.make_async_copy(x_hbm.at[k], xr.at[slot, pl.ds(half * T, T)], ld_sem.at[slot, half])

    load_own(0, 0, 0).start()
    pl.semaphore_wait(barrier, 3)

    @pl.loop(0, NCH)
    def _(k):
        for which, dev in enumerate((partner, nbr_x, nbr_y)):
            for copy in send_own(k, which, dev):
                copy.start()

    load_own(1, 1, 0).start()

    @pl.loop(0, NCH)
    def _(k):
        slot = lax.rem(k, 2)
        load_own(k, slot, 0).wait()
        norm = jnp.zeros((1, T), jnp.float32)
        for h in range(2):
            part = xr[slot, :T, h * T : (h + 1) * T].astype(jnp.float32).T
            norm = norm + jnp.sum(part * part, axis=0, keepdims=True)
            scaled = (part * -2.0).astype(jnp.bfloat16)
            for side in range(2):
                xt[k, side, h * T : (h + 1) * T, :] = scaled[:, side * 128 : (side + 1) * 128]
        ni[k] = jnp.broadcast_to(norm, (8, T))

        @pl.when(k + 2 < NCH)
        def _():
            load_own(k + 2, slot, 0).start()

    own_v.wait()
    load_own(0, 0, 0).start()
    load_own(1, 0, 1).start()

    scale = jnp.full((1, 128), ls_ref[0], jnp.float32)
    rate = -math.log2(math.e) / (2.0 * scale * scale)
    amp = jnp.full((1, 128), os_ref[0], jnp.float32)

    @pl.loop(0, NCH)
    def _(k):
        ysum[k] = jnp.zeros((COLS, T), jnp.float32)

    def write_k(t, parity):
        streamed, number, slot = stream_of(t)

        @pl.when(streamed)
        def _():
            pltpu.make_async_copy(stage.at[parity], kst.at[number], kw_sem.at[parity]).start()

        @pl.when(jnp.logical_not(streamed))
        def _():
            pltpu.make_async_copy(stage.at[parity], kept.at[slot], kw_sem.at[parity]).start()

    def written(parity):
        pltpu.make_async_copy(stage.at[parity], kst.at[0], kw_sem.at[parity]).wait()

    def read_k(number):
        slot = lax.rem(number, RING)
        return pltpu.make_async_copy(kst.at[number], stage.at[slot], kr_sem.at[slot])

    def weigh(x_slot, parity, i):
        gram_tile = jnp.dot(xr[x_slot], wide(xt[i, 0], xt[i, 1]), preferred_element_type=jnp.float32)
        for h in range(2):
            lanes = slice(h * 128, (h + 1) * 128)
            dist = jnp.maximum((nj[...] + ni[i, 0:1, lanes]) + gram_tile[:, lanes], 0.0)
            stage[parity, i, h] = (amp * jnp.exp2(dist * rate)).astype(jnp.bfloat16)

    def apply(source, slot, lhs, i):
        ysum[i] += jnp.dot(lhs, wide(source[slot, i, 0], source[slot, i, 1]), preferred_element_type=jnp.float32)

    def pair_of(table, t):
        rel, k = chunk_of(2 * t)
        rel_2, k_2 = chunk_of(2 * t + 1)
        return jnp.concatenate([table[rel, k], table[rel_2, k_2]], axis=1)

    def fetch(s):
        rel, k = chunk_of(s)
        half = lax.rem(s, 2)
        slot = lax.rem(lax.div(s, 2), XR)

        @pl.when(rel == 0)
        def _():
            load_own(k, slot, half).start()

        @pl.when(rel > 0)
        def _():
            remote(xall.at[rel, k], xall.at[rel, k], so_x.at[0, 0], rx_sem.at[rel, k], partner).wait_recv()
            remote(vt.at[rel, k], vt.at[rel, k], so_v.at[0, 0], rv_sem.at[rel, k], partner).wait_recv()
            pltpu.make_async_copy(
                xall.at[rel, k], xr.at[slot, pl.ds(half * T, T)], ld_sem.at[slot, half]
            ).start()

        @pl.when(jnp.logical_and(rel >= 2, lax.rem(rel, 2) == 0))
        def _():
            for copy in forward_partner(rel, k):
                copy.start()

        @pl.when(jnp.logical_and(rel == 2, lax.rem(k, 2) == 1))
        def _():
            for copy in forward_nbr(2, k, nbr_y):
                copy.start()

        @pl.when(jnp.logical_and(rel == 4, lax.rem(k, 2) == 0))
        def _():
            for copy in forward_nbr(4, k, nbr_x):
                copy.start()

    def trip(t, parity, place):
        if place < 2:
            fetch(2 * t + 2)
            fetch(2 * t + 3)
        if place > 0:
            write_k(t - 1, 1 - parity)

            @pl.when(t >= 2)
            def _():
                written(parity)

        x_slot = parity
        load_own(0, x_slot, 0).wait()
        load_own(0, x_slot, 1).wait()
        for p in range(2 * NP):
            rows = slice(p * PIECE, (p + 1) * PIECE)
            part = xr[x_slot, rows, :].astype(jnp.float32)
            norm = jnp.sum(part * part, axis=1, keepdims=True)
            nj[rows, :] = jnp.broadcast_to(norm, (PIECE, 128))
        if place > 0:
            lhs = pair_of(vt, t - 1)
        for i in range(NCH):
            if place > 0:
                apply(stage, 1 - parity, lhs, i)
            weigh(x_slot, parity, i)

    trip(jnp.int32(0), 0, 0)

    for lo, hi in ((0, 6), (6, 15), (15, PAIRS // 2 - 1)):
        with jax.named_scope(f"first_{lo}"):

            @pl.loop(lo, hi)
            def _(m):
                trip(2 * m + 1, 1, 1)
                trip(2 * m + 2, 0, 1)

    trip(jnp.int32(PAIRS - 1), 1, 2)
    write_k(jnp.int32(PAIRS - 1), 1)
    lhs = pair_of(vt, jnp.int32(PAIRS - 1))
    for i in range(NCH):
        apply(stage, 1, lhs, i)

    @pl.loop(0, NCH)
    def _(k):
        yall[0, k] = ysum[k].astype(jnp.bfloat16)
        ysum[k] = jnp.zeros((COLS, T), jnp.float32)

    @pl.loop(0, NCH)
    def _(k):
        for which, dev in enumerate((partner, nbr_x, nbr_y)):
            for copy in send_own(k, which, dev):
                copy.wait_send()
        for rel in (2, 4, 6):
            for copy in forward_partner(rel, k):
                copy.wait_send()
        for copy in forward_nbr(2, k, nbr_y):
            copy.wait_send()

    half = NCH // 2

    def y_copy(src_rel, dst_rel, lo, n, idx, dev):
        return remote(
            yall.at[src_rel, pl.ds(lo, n)], yall.at[dst_rel, pl.ds(lo, n)], ys_sem.at[idx], yr_sem.at[idx], dev
        )

    y_moves = (
        (0, 1, 0, NCH, partner),
        (0, 2, 0, NCH, nbr_x),
        (0, 4, 0, NCH, nbr_y),
        (2, 3, 0, NCH, partner),
        (4, 5, 0, NCH, partner),
        (4, 6, 0, half, nbr_x),
        (2, 6, half, half, nbr_y),
        (6, 7, 0, NCH, partner),
    )

    def y_move(idx):
        src, dst, lo, n, dev = y_moves[idx]
        return y_copy(src, dst, lo, n, idx, dev)

    def y_arrived(idx):
        _, dst, lo, n, dev = y_moves[idx]
        return y_copy(dst, dst, lo, n, idx, dev)

    for idx in range(3):
        y_move(idx).start()

    for parity in range(2):
        written(parity)
    for number in range(RING):
        read_k(jnp.int32(number)).start()

    def second(t):
        s = 2 * t

        @pl.when(s == 12)
        def _():
            y_arrived(0).wait_recv()

        @pl.when(s == 20)
        def _():
            y_arrived(1).wait_recv()
            y_arrived(2).wait_recv()
            for idx in range(3, 7):
                y_move(idx).start()

        @pl.when(s == 28)
        def _():
            y_arrived(3).wait_recv()
            y_arrived(4).wait_recv()

        @pl.when(s == 56)
        def _():
            y_arrived(5).wait_recv()
            y_arrived(6).wait_recv()
            y_move(7).start()

        @pl.when(s == 70)
        def _():
            y_arrived(7).wait_recv()

        streamed, number, slot = stream_of(t)

        @pl.when(streamed)
        def _():
            read_k(number).wait()

        lhs = pair_of(yall, t)

        @pl.when(streamed)
        def _():
            for i in range(NCH):
                apply(stage, lax.rem(number, RING), lhs, i)

        @pl.when(jnp.logical_not(streamed))
        def _():
            for i in range(NCH):
                apply(kept, slot, lhs, i)

        @pl.when(jnp.logical_and(streamed, number + RING < N_STREAM))
        def _():
            read_k(number + RING).start()

    for lo, hi in ((0, 12), (12, 24), (24, 48)):
        with jax.named_scope(f"second_{lo}"):

            @pl.loop(lo, hi)
            def _(t):
                second(t)

    for idx in range(8):
        y_move(idx).wait_send()

    @pl.loop(0, NCH)
    def _(k):
        out_ref[k] = ysum[k]


def solution(mesh):
    rows = NCH * T

    def local_program(x_loc, v_loc, length_scale, out_scale):
        vt_loc = v_loc.reshape(NCH, T, COLS).transpose(0, 2, 1)
        dma = pltpu.SemaphoreType.DMA
        out, _, _ = pl.pallas_call(
            body,
            out_shape=(
                jax.ShapeDtypeStruct((NCH, COLS, T), jnp.float32),
                jax.ShapeDtypeStruct((NREL, NCH, T, FEAT), jnp.bfloat16),
                jax.ShapeDtypeStruct((N_STREAM, NCH, 2, 2 * T, 128), jnp.bfloat16),
            ),
            in_specs=[
                pl.BlockSpec(memory_space=pltpu.HBM),
                pl.BlockSpec(memory_space=pltpu.HBM),
                pl.BlockSpec(memory_space=pltpu.SMEM),
                pl.BlockSpec(memory_space=pltpu.SMEM),
            ],
            out_specs=(
                pl.BlockSpec(memory_space=pltpu.VMEM),
                pl.BlockSpec(memory_space=pltpu.HBM),
                pl.BlockSpec(memory_space=pltpu.HBM),
            ),
            scratch_shapes=[
                pltpu.VMEM((NCH, 2, FEAT, 128), jnp.bfloat16),
                pltpu.VMEM((NREL, NCH, COLS, T), jnp.bfloat16),
                pltpu.VMEM((NREL, NCH, COLS, T), jnp.bfloat16),
                pltpu.VMEM((N_RES, NCH, 2, 2 * T, 128), jnp.bfloat16),
                pltpu.VMEM((RING, NCH, 2, 2 * T, 128), jnp.bfloat16),
                pltpu.VMEM((XR, 2 * T, FEAT), jnp.bfloat16),
                pltpu.VMEM((2 * T, 128), jnp.float32),
                pltpu.VMEM((NCH, 8, T), jnp.float32),
                dma((XR, 2)), dma((2,)), dma((RING,)), dma,
                dma((NREL, NCH)), dma((NREL, NCH)),
                dma((3, NCH)), dma((3, NCH)),
                dma((3, NCH)), dma((3, NCH)),
                dma((NCH,)), dma((NCH,)),
                dma((8,)), dma((8,)),
                pltpu.VMEM((NCH, COLS, T), jnp.float32),
            ],
            compiler_params=pltpu.CompilerParams(
                collective_id=0, has_side_effects=True, vmem_limit_bytes=67_043_328
            ),
        )(x_loc.reshape(NCH, T, FEAT), vt_loc, length_scale, out_scale)
        return out.transpose(0, 2, 1).reshape(rows, COLS)

    row_spec = P(("task", "row"), None)
    return jax.shard_map(
        local_program,
        mesh=mesh,
        in_specs=(row_spec, row_spec, P("task"), P("task")),
        out_specs=row_spec,
        check_vma=False,
    )
```

```python
import functools
import math

import jax
import jax.numpy as jnp
from jax import lax
from jax.experimental import pallas as pl
from jax.experimental.pallas import tpu as pltpu
from jax.sharding import PartitionSpec as P

MESH = pl.DeviceIdType.MESH
T = 256
FEAT = 512
COLS = 64
NCH = 12
NREL = 8
STEPS = NREL * NCH
PIECE = 64
NP = T // PIECE
NI = NCH // 2
PAIRS = STEPS // 2
RES_IN, RES_OF = 2, 5
N_RES = (PAIRS - 12) // RES_OF * RES_IN
RING = 3
N_STREAM = PAIRS - N_RES
XR = 2


def chunk_of(s):
    j = lax.rem(s + 2, 4)
    v = lax.div(s - 22, 4) - 1
    late = jnp.where(s < 26, 0, jnp.where(s >= 94, 1, lax.div(j, 2)))
    group = jnp.where(s < 26, 0, jnp.where(s >= 94, 17, v + 1 - late))
    side = lax.rem(s, 2)
    far = group >= 12
    rel = jnp.where(far, 6, 2 + 2 * side) + late
    chunk = jnp.where(far, 2 * (group - 12) + side, group)
    near_rel = lax.div(s, NCH)
    near_chunk = lax.rem(s, NCH)
    return jnp.where(s < 24, near_rel, rel), jnp.where(s < 24, near_chunk, chunk)


def wide(left, right):
    return jnp.concatenate([left, right], axis=1)


def stream_of(t):
    u = jnp.maximum(t - 12, 0)
    w = lax.rem(u, RES_OF)
    o = lax.div(u, RES_OF)
    keep = jnp.where(o == (PAIRS - 12) // RES_OF, 0, RES_IN)
    streamed = jnp.logical_or(t < 12, w >= keep)
    number = jnp.where(t < 12, t, 12 + o * (RES_OF - RES_IN) + w - keep)
    return streamed, number, o * RES_IN + w


def body(
    x_hbm, vt_hbm, ls_ref, os_ref,
    out_ref, xall, kst,
    xt, vt, yall, kept, stage, xr, nj, ni,
    ld_sem, kw_sem, kr_sem, vl_sem,
    rx_sem, rv_sem, so_x, so_v, sp_x, sp_v, sn_x, sn_v, ys_sem, yr_sem,
    ysum, consts, su_sem,
):
    me = lax.axis_index("row")
    partner = me + 1 - 2 * lax.rem(me, 2)
    nbr_x = me + 2 - 4 * lax.rem(lax.div(me, 2), 2)
    nbr_y = me + 4 - 8 * lax.div(me, 4)

    def remote(src, dst, ss, rs, dev):
        return pltpu.make_async_remote_copy(
            src_ref=src, dst_ref=dst, send_sem=ss, recv_sem=rs, device_id={"row": dev}, device_id_type=MESH
        )

    def send_own(k, which, dev):
        slot = (1, 2, 4)[which]
        return (
            remote(x_hbm.at[k], xall.at[slot, k], so_x.at[which, k], rx_sem.at[slot, k], dev),
            remote(vt_hbm.at[k], vt.at[slot, k], so_v.at[which, k], rv_sem.at[slot, k], dev),
        )

    def forward_partner(rel, k):
        row = lax.div(rel, 2) - 1
        return (
            remote(xall.at[rel, k], xall.at[rel + 1, k], sp_x.at[row, k], rx_sem.at[rel + 1, k], partner),
            remote(vt.at[rel, k], vt.at[rel + 1, k], sp_v.at[row, k], rv_sem.at[rel + 1, k], partner),
        )

    def forward_nbr(rel, k, dev):
        return (
            remote(xall.at[rel, k], xall.at[6, k], sn_x.at[k], rx_sem.at[6, k], dev),
            remote(vt.at[rel, k], vt.at[6, k], sn_v.at[k], rv_sem.at[6, k], dev),
        )

    barrier = pltpu.get_barrier_semaphore()
    for dev in (partner, nbr_x, nbr_y):
        pl.semaphore_signal(barrier, inc=1, device_id={"row": dev}, device_id_type=MESH)

    own_v = pltpu.make_async_copy(vt_hbm, vt.at[0], vl_sem)
    own_v.start()

    def load_own(k, slot, half):
        return pltpu.make_async_copy(x_hbm.at[k], xr.at[slot, pl.ds(half * T, T)], ld_sem.at[slot, half])

    @pl.loop(0, NCH)
    def _(k):
        for q in range(4):
            pltpu.make_async_copy(
                x_hbm.at[k, :, pl.ds(q * 128, 128)],
                stage.at[RING - 1, k, q // 2, pl.ds(q % 2 * T, T)],
                su_sem.at[k],
            ).start()

    load_own(0, 0, 0).start()
    load_own(1, 0, 1).start()
    pl.semaphore_wait(barrier, 3)

    @pl.loop(0, NCH)
    def _(k):
        for which, dev in enumerate((partner, nbr_x, nbr_y)):
            for copy in send_own(k, which, dev):
                copy.start()

    @pl.loop(0, NCH)
    def _(k):
        pltpu.make_async_copy(x_hbm.at[k], xr.at[1, pl.ds(0, T)], su_sem.at[k]).wait()
        norm = jnp.zeros((1, T), jnp.float32)
        for q in range(4):
            part = stage[RING - 1, k, q // 2, q % 2 * T : (q % 2 + 1) * T, :].astype(jnp.float32).T
            norm = norm + jnp.sum(part * part, axis=0, keepdims=True)
            scaled = (part * -2.0).astype(jnp.bfloat16)
            for side in range(2):
                xt[k, side, q * 128 : (q + 1) * 128, :] = scaled[:, side * 128 : (side + 1) * 128]
        ni[k] = jnp.broadcast_to(norm, (8, T))

    own_v.wait()

    scale = jnp.full((8, 128), ls_ref[0], jnp.float32)
    consts[0] = -math.log2(math.e) / (2.0 * scale * scale)
    consts[1] = jnp.full((8, 128), os_ref[0], jnp.float32)

    @pl.loop(0, NCH)
    def _(k):
        ysum[k] = jnp.zeros((COLS, T), jnp.float32)

    def write_k(t, parity):
        streamed, number, slot = stream_of(t)

        @pl.when(streamed)
        def _():
            pltpu.make_async_copy(stage.at[parity], kst.at[number], kw_sem.at[parity]).start()

        @pl.when(jnp.logical_not(streamed))
        def _():
            pltpu.make_async_copy(stage.at[parity], kept.at[slot], kw_sem.at[parity]).start()

    def written(parity):
        pltpu.make_async_copy(stage.at[parity], kst.at[0], kw_sem.at[parity]).wait()

    def read_k(number):
        slot = lax.rem(number, RING)
        return pltpu.make_async_copy(kst.at[number], stage.at[slot], kr_sem.at[slot])

    def weigh(x_slot, parity, i):
        gram_tile = jnp.dot(xr[x_slot], wide(xt[i, 0], xt[i, 1]), preferred_element_type=jnp.float32)
        for h in range(2):
            lanes = slice(h * 128, (h + 1) * 128)
            dist = jnp.maximum((nj[...] + ni[i, 0:1, lanes]) + gram_tile[:, lanes], 0.0)
            stage[parity, i, h] = (consts[1, 0:1, :] * jnp.exp2(dist * consts[0, 0:1, :])).astype(jnp.bfloat16)

    def apply(source, slot, lhs, i):
        ysum[i] += jnp.dot(lhs, wide(source[slot, i, 0], source[slot, i, 1]), preferred_element_type=jnp.float32)

    def pair_of(table, t):
        rel, k = chunk_of(2 * t)
        rel_2, k_2 = chunk_of(2 * t + 1)
        return jnp.concatenate([table[rel, k], table[rel_2, k_2]], axis=1)

    def fetch(s):
        rel, k = chunk_of(s)
        half = lax.rem(s, 2)
        slot = lax.rem(lax.div(s, 2), XR)

        @pl.when(rel == 0)
        def _():
            load_own(k, slot, half).start()

        @pl.when(rel > 0)
        def _():
            remote(xall.at[rel, k], xall.at[rel, k], so_x.at[0, 0], rx_sem.at[rel, k], partner).wait_recv()
            remote(vt.at[rel, k], vt.at[rel, k], so_v.at[0, 0], rv_sem.at[rel, k], partner).wait_recv()
            pltpu.make_async_copy(
                xall.at[rel, k], xr.at[slot, pl.ds(half * T, T)], ld_sem.at[slot, half]
            ).start()

        @pl.when(jnp.logical_and(rel >= 2, lax.rem(rel, 2) == 0))
        def _():
            for copy in forward_partner(rel, k):
                copy.start()

        @pl.when(jnp.logical_and(rel == 2, lax.rem(k, 2) == 1))
        def _():
            for copy in forward_nbr(2, k, nbr_y):
                copy.start()

        @pl.when(jnp.logical_and(rel == 4, lax.rem(k, 2) == 0))
        def _():
            for copy in forward_nbr(4, k, nbr_x):
                copy.start()

    def trip(t, parity, place):
        if place < 2:
            fetch(2 * t + 2)
            fetch(2 * t + 3)
        if place > 0:
            write_k(t - 1, 1 - parity)

            @pl.when(t >= 2)
            def _():
                written(parity)

        x_slot = parity
        load_own(0, x_slot, 0).wait()
        load_own(0, x_slot, 1).wait()
        for p in range(2 * NP):
            rows = slice(p * PIECE, (p + 1) * PIECE)
            part = xr[x_slot, rows, :].astype(jnp.float32)
            norm = jnp.sum(part * part, axis=1, keepdims=True)
            nj[rows, :] = jnp.broadcast_to(norm, (PIECE, 128))
        if place > 0:
            lhs = pair_of(vt, t - 1)
        for i in range(NCH + 4):
            if place > 0 and i >= 4:
                apply(stage, 1 - parity, lhs, i - 4)
            if i < NCH:
                weigh(x_slot, parity, i)

    trip(jnp.int32(0), 0, 0)

    @pl.loop(0, PAIRS // 2 - 1)
    def _(m):
        trip(2 * m + 1, 1, 1)
        trip(2 * m + 2, 0, 1)

    trip(jnp.int32(PAIRS - 1), 1, 2)
    write_k(jnp.int32(PAIRS - 1), 1)
    lhs = pair_of(vt, jnp.int32(PAIRS - 1))
    for i in range(NCH):
        apply(stage, 1, lhs, i)

    @pl.loop(0, NCH)
    def _(k):
        yall[0, k] = ysum[k].astype(jnp.bfloat16)
        ysum[k] = jnp.zeros((COLS, T), jnp.float32)

    @pl.loop(0, NCH)
    def _(k):
        for which, dev in enumerate((partner, nbr_x, nbr_y)):
            for copy in send_own(k, which, dev):
                copy.wait_send()
        for rel in (2, 4, 6):
            for copy in forward_partner(rel, k):
                copy.wait_send()
        for copy in forward_nbr(2, k, nbr_y):
            copy.wait_send()

    half = NCH // 2

    def y_copy(src_rel, dst_rel, lo, n, idx, dev):
        return remote(
            yall.at[src_rel, pl.ds(lo, n)], yall.at[dst_rel, pl.ds(lo, n)], ys_sem.at[idx], yr_sem.at[idx], dev
        )

    y_moves = (
        (0, 1, 0, NCH, partner),
        (0, 2, 0, NCH, nbr_x),
        (0, 4, 0, NCH, nbr_y),
        (2, 3, 0, NCH, partner),
        (4, 5, 0, NCH, partner),
        (4, 6, 0, half, nbr_x),
        (2, 6, half, half, nbr_y),
        (6, 7, 0, NCH, partner),
    )

    def y_move(idx):
        src, dst, lo, n, dev = y_moves[idx]
        return y_copy(src, dst, lo, n, idx, dev)

    def y_arrived(idx):
        _, dst, lo, n, dev = y_moves[idx]
        return y_copy(dst, dst, lo, n, idx, dev)

    for idx in range(3):
        y_move(idx).start()

    for parity in range(2):
        written(parity)
    for number in range(RING):
        read_k(jnp.int32(number)).start()

    def second(t):
        s = 2 * t

        @pl.when(s == 12)
        def _():
            y_arrived(0).wait_recv()

        @pl.when(s == 22)
        def _():
            y_arrived(1).wait_recv()
            y_arrived(2).wait_recv()
            for idx in range(3, 7):
                y_move(idx).start()

        @pl.when(s == 28)
        def _():
            y_arrived(3).wait_recv()
            y_arrived(4).wait_recv()

        @pl.when(s == 56)
        def _():
            y_arrived(5).wait_recv()
            y_arrived(6).wait_recv()
            y_move(7).start()

        @pl.when(s == 70)
        def _():
            y_arrived(7).wait_recv()

        streamed, number, slot = stream_of(t)

        @pl.when(streamed)
        def _():
            read_k(number).wait()

        lhs = pair_of(yall, t)

        @pl.when(streamed)
        def _():
            for i in range(NCH):
                apply(stage, lax.rem(number, RING), lhs, i)

        @pl.when(jnp.logical_not(streamed))
        def _():
            for i in range(NCH):
                apply(kept, slot, lhs, i)

        @pl.when(jnp.logical_and(streamed, number + RING < N_STREAM))
        def _():
            read_k(number + RING).start()

    @pl.loop(0, PAIRS)
    def _(t):
        second(t)

    for idx in range(8):
        y_move(idx).wait_send()

    @pl.loop(0, NCH)
    def _(k):
        out_ref[k] = ysum[k]


def solution(mesh):
    rows = NCH * T

    def local_program(x_loc, v_loc, length_scale, out_scale):
        vt_loc = v_loc.reshape(NCH, T, COLS).transpose(0, 2, 1)
        dma = pltpu.SemaphoreType.DMA
        out, _, _ = pl.pallas_call(
            body,
            out_shape=(
                jax.ShapeDtypeStruct((NCH, COLS, T), jnp.float32),
                jax.ShapeDtypeStruct((NREL, NCH, T, FEAT), jnp.bfloat16),
                jax.ShapeDtypeStruct((N_STREAM, NCH, 2, 2 * T, 128), jnp.bfloat16),
            ),
            in_specs=[
                pl.BlockSpec(memory_space=pltpu.HBM),
                pl.BlockSpec(memory_space=pltpu.HBM),
                pl.BlockSpec(memory_space=pltpu.SMEM),
                pl.BlockSpec(memory_space=pltpu.SMEM),
            ],
            out_specs=(
                pl.BlockSpec(memory_space=pltpu.VMEM),
                pl.BlockSpec(memory_space=pltpu.HBM),
                pl.BlockSpec(memory_space=pltpu.HBM),
            ),
            scratch_shapes=[
                pltpu.VMEM((NCH, 2, FEAT, 128), jnp.bfloat16),
                pltpu.VMEM((NREL, NCH, COLS, T), jnp.bfloat16),
                pltpu.VMEM((NREL, NCH, COLS, T), jnp.bfloat16),
                pltpu.VMEM((N_RES, NCH, 2, 2 * T, 128), jnp.bfloat16),
                pltpu.VMEM((RING, NCH, 2, 2 * T, 128), jnp.bfloat16),
                pltpu.VMEM((XR, 2 * T, FEAT), jnp.bfloat16),
                pltpu.VMEM((2 * T, 128), jnp.float32),
                pltpu.VMEM((NCH, 8, T), jnp.float32),
                dma((XR, 2)), dma((2,)), dma((RING,)), dma,
                dma((NREL, NCH)), dma((NREL, NCH)),
                dma((3, NCH)), dma((3, NCH)),
                dma((3, NCH)), dma((3, NCH)),
                dma((NCH,)), dma((NCH,)),
                dma((8,)), dma((8,)),
                pltpu.VMEM((NCH, COLS, T), jnp.float32),
                pltpu.VMEM((2, 8, 128), jnp.float32),
                dma((NCH,)),
            ],
            compiler_params=pltpu.CompilerParams(
                collective_id=0,
                has_side_effects=True,
                vmem_limit_bytes=67_043_328
            ),
        )(x_loc.reshape(NCH, T, FEAT), vt_loc, length_scale, out_scale)
        return out.transpose(0, 2, 1).reshape(rows, COLS)

    row_spec = P(("task", "row"), None)
    return jax.shard_map(
        local_program,
        mesh=mesh,
        in_specs=(row_spec, row_spec, P("task"), P("task")),
        out_specs=row_spec,
        check_vma=False,
    )
```

```python
import functools
import math

import jax
import jax.numpy as jnp
from jax import lax
from jax.experimental import pallas as pl
from jax.experimental.pallas import tpu as pltpu
from jax.sharding import PartitionSpec as P

MESH = pl.DeviceIdType.MESH
T = 256
FEAT = 512
COLS = 64
NCH = 12
NREL = 8
STEPS = NREL * NCH
PIECE = 64
NP = T // PIECE
NI = NCH // 2
PAIRS = STEPS // 2
RES_IN, RES_OF = 2, 5
N_RES = (PAIRS - 12) // RES_OF * RES_IN
RING = 3
N_STREAM = PAIRS - N_RES
XR = 2


def split(n, by, factor, power):
    whole = lax.div(n * factor, power)
    return whole, n - whole * by


def chunk_of(s):
    j = lax.rem(s + 2, 4)
    v = lax.div(s - 22, 4) - 1
    late = jnp.where(s < 26, 0, jnp.where(s >= 94, 1, lax.div(j, 2)))
    group = jnp.where(s < 26, 0, jnp.where(s >= 94, 17, v + 1 - late))
    side = lax.rem(s, 2)
    far = group >= 12
    rel = jnp.where(far, 6, 2 + 2 * side) + late
    chunk = jnp.where(far, 2 * (group - 12) + side, group)
    near_rel, near_chunk = split(s, NCH, 43, 512)
    return jnp.where(s < 24, near_rel, rel), jnp.where(s < 24, near_chunk, chunk)


def wide(left, right):
    return jnp.concatenate([left, right], axis=1)


def stream_of(t):
    u = jnp.maximum(t - 12, 0)
    o, w = split(u, RES_OF, 205, 1024)
    keep = jnp.where(o == (PAIRS - 12) // RES_OF, 0, RES_IN)
    streamed = jnp.logical_or(t < 12, w >= keep)
    number = jnp.where(t < 12, t, 12 + o * (RES_OF - RES_IN) + w - keep)
    return streamed, number, o * RES_IN + w


def body(
    x_hbm, vt_hbm, ls_ref, os_ref,
    out_ref, xall, kst,
    xt, vt, yall, kept, stage, xr, nj, ni,
    ld_sem, kw_sem, kr_sem, vl_sem,
    rx_sem, rv_sem, so_x, so_v, sp_x, sp_v, sn_x, sn_v, ys_sem, yr_sem,
    ysum, consts, su_sem,
):
    me = lax.axis_index("row")
    partner = me + 1 - 2 * lax.rem(me, 2)
    nbr_x = me + 2 - 4 * lax.rem(lax.div(me, 2), 2)
    nbr_y = me + 4 - 8 * lax.div(me, 4)

    def remote(src, dst, ss, rs, dev):
        return pltpu.make_async_remote_copy(
            src_ref=src, dst_ref=dst, send_sem=ss, recv_sem=rs, device_id={"row": dev}, device_id_type=MESH
        )

    def send_own(k, which, dev):
        slot = (1, 2, 4)[which]
        return (
            remote(x_hbm.at[k], xall.at[slot, k], so_x.at[which, k], rx_sem.at[slot, k], dev),
            remote(vt_hbm.at[k], vt.at[slot, k], so_v.at[which, k], rv_sem.at[slot, k], dev),
        )

    def forward_partner(rel, k):
        row = lax.div(rel, 2) - 1
        return (
            remote(xall.at[rel, k], xall.at[rel + 1, k], sp_x.at[row, k], rx_sem.at[rel + 1, k], partner),
            remote(vt.at[rel, k], vt.at[rel + 1, k], sp_v.at[row, k], rv_sem.at[rel + 1, k], partner),
        )

    def forward_nbr(rel, k, dev):
        return (
            remote(xall.at[rel, k], xall.at[6, k], sn_x.at[k], rx_sem.at[6, k], dev),
            remote(vt.at[rel, k], vt.at[6, k], sn_v.at[k], rv_sem.at[6, k], dev),
        )

    barrier = pltpu.get_barrier_semaphore()
    for dev in (partner, nbr_x, nbr_y):
        pl.semaphore_signal(barrier, inc=1, device_id={"row": dev}, device_id_type=MESH)

    own_v = pltpu.make_async_copy(vt_hbm, vt.at[0], vl_sem)
    own_v.start()

    def load_own(k, slot, half):
        return pltpu.make_async_copy(x_hbm.at[k], xr.at[slot, pl.ds(half * T, T)], ld_sem.at[slot, half])

    @pl.loop(0, NCH)
    def _(k):
        for q in range(4):
            pltpu.make_async_copy(
                x_hbm.at[k, :, pl.ds(q * 128, 128)],
                stage.at[RING - 1, k, q // 2, pl.ds(q % 2 * T, T)],
                su_sem.at[k],
            ).start()

    load_own(0, 0, 0).start()
    load_own(1, 0, 1).start()
    pl.semaphore_wait(barrier, 3)

    @pl.loop(0, NCH)
    def _(k):
        for which, dev in enumerate((partner, nbr_x, nbr_y)):
            for copy in send_own(k, which, dev):
                copy.start()

    @pl.loop(0, NCH)
    def _(k):
        pltpu.make_async_copy(x_hbm.at[k], xr.at[1, pl.ds(0, T)], su_sem.at[k]).wait()
        norm = jnp.zeros((1, T), jnp.float32)
        for q in range(4):
            part = stage[RING - 1, k, q // 2, q % 2 * T : (q % 2 + 1) * T, :].astype(jnp.float32).T
            norm = norm + jnp.sum(part * part, axis=0, keepdims=True)
            scaled = (part * -2.0).astype(jnp.bfloat16)
            for side in range(2):
                xt[k, side, q * 128 : (q + 1) * 128, :] = scaled[:, side * 128 : (side + 1) * 128]
        ni[k] = jnp.broadcast_to(norm, (8, T))

    own_v.wait()

    scale = jnp.full((8, 128), ls_ref[0], jnp.float32)
    consts[0] = -math.log2(math.e) / (2.0 * scale * scale)
    consts[1] = jnp.full((8, 128), os_ref[0], jnp.float32)

    @pl.loop(0, NCH)
    def _(k):
        ysum[k] = jnp.zeros((COLS, T), jnp.float32)

    def write_k(t, parity):
        streamed, number, slot = stream_of(t)

        @pl.when(streamed)
        def _():
            pltpu.make_async_copy(stage.at[parity], kst.at[number], kw_sem.at[parity]).start()

        @pl.when(jnp.logical_not(streamed))
        def _():
            pltpu.make_async_copy(stage.at[parity], kept.at[slot], kw_sem.at[parity]).start()

    def written(parity):
        pltpu.make_async_copy(stage.at[parity], kst.at[0], kw_sem.at[parity]).wait()

    def read_k(number):
        _, slot = split(number, RING, 171, 512)
        return pltpu.make_async_copy(kst.at[number], stage.at[slot], kr_sem.at[slot])

    def weigh(x_slot, parity, i):
        gram_tile = jnp.dot(xr[x_slot], wide(xt[i, 0], xt[i, 1]), preferred_element_type=jnp.float32)
        for h in range(2):
            lanes = slice(h * 128, (h + 1) * 128)
            dist = jnp.maximum((nj[...] + ni[i, 0:1, lanes]) + gram_tile[:, lanes], 0.0)
            stage[parity, i, h] = (consts[1, 0:1, :] * jnp.exp2(dist * consts[0, 0:1, :])).astype(jnp.bfloat16)

    def apply(source, slot, lhs, i):
        ysum[i] += jnp.dot(lhs, wide(source[slot, i, 0], source[slot, i, 1]), preferred_element_type=jnp.float32)

    def pair_of(table, t):
        rel, k = chunk_of(2 * t)
        rel_2, k_2 = chunk_of(2 * t + 1)
        return jnp.concatenate([table[rel, k], table[rel_2, k_2]], axis=1)

    def fetch(s):
        rel, k = chunk_of(s)
        half = lax.rem(s, 2)
        slot = lax.rem(lax.div(s, 2), XR)

        @pl.when(rel == 0)
        def _():
            load_own(k, slot, half).start()

        @pl.when(rel > 0)
        def _():
            remote(xall.at[rel, k], xall.at[rel, k], so_x.at[0, 0], rx_sem.at[rel, k], partner).wait_recv()
            remote(vt.at[rel, k], vt.at[rel, k], so_v.at[0, 0], rv_sem.at[rel, k], partner).wait_recv()
            pltpu.make_async_copy(
                xall.at[rel, k], xr.at[slot, pl.ds(half * T, T)], ld_sem.at[slot, half]
            ).start()

        @pl.when(jnp.logical_and(rel >= 2, lax.rem(rel, 2) == 0))
        def _():
            for copy in forward_partner(rel, k):
                copy.start()

        @pl.when(jnp.logical_and(rel == 2, lax.rem(k, 2) == 1))
        def _():
            for copy in forward_nbr(2, k, nbr_y):
                copy.start()

        @pl.when(jnp.logical_and(rel == 4, lax.rem(k, 2) == 0))
        def _():
            for copy in forward_nbr(4, k, nbr_x):
                copy.start()

    def trip(t, parity, place):
        if place < 2:
            fetch(2 * t + 2)
            fetch(2 * t + 3)
        if place > 0:
            write_k(t - 1, 1 - parity)

            @pl.when(t >= 2)
            def _():
                written(parity)

        x_slot = parity
        load_own(0, x_slot, 0).wait()
        load_own(0, x_slot, 1).wait()
        for p in range(2 * NP):
            rows = slice(p * PIECE, (p + 1) * PIECE)
            part = xr[x_slot, rows, :].astype(jnp.float32)
            norm = jnp.sum(part * part, axis=1, keepdims=True)
            nj[rows, :] = jnp.broadcast_to(norm, (PIECE, 128))
        if place > 0:
            lhs = pair_of(vt, t - 1)
        for i in range(NCH + 4):
            if place > 0 and i >= 4:
                apply(stage, 1 - parity, lhs, i - 4)
            if i < NCH:
                weigh(x_slot, parity, i)

    trip(jnp.int32(0), 0, 0)

    @pl.loop(0, PAIRS // 2 - 1)
    def _(m):
        trip(2 * m + 1, 1, 1)
        trip(2 * m + 2, 0, 1)

    trip(jnp.int32(PAIRS - 1), 1, 2)
    write_k(jnp.int32(PAIRS - 1), 1)
    lhs = pair_of(vt, jnp.int32(PAIRS - 1))
    for i in range(NCH):
        apply(stage, 1, lhs, i)

    @pl.loop(0, NCH)
    def _(k):
        yall[0, k] = ysum[k].astype(jnp.bfloat16)
        ysum[k] = jnp.zeros((COLS, T), jnp.float32)

    @pl.loop(0, NCH)
    def _(k):
        for which, dev in enumerate((partner, nbr_x, nbr_y)):
            for copy in send_own(k, which, dev):
                copy.wait_send()
        for rel in (2, 4, 6):
            for copy in forward_partner(rel, k):
                copy.wait_send()
        for copy in forward_nbr(2, k, nbr_y):
            copy.wait_send()

    half = NCH // 2

    def y_copy(src_rel, dst_rel, lo, n, idx, dev):
        return remote(
            yall.at[src_rel, pl.ds(lo, n)], yall.at[dst_rel, pl.ds(lo, n)], ys_sem.at[idx], yr_sem.at[idx], dev
        )

    y_moves = (
        (0, 1, 0, NCH, partner),
        (0, 2, 0, NCH, nbr_x),
        (0, 4, 0, NCH, nbr_y),
        (2, 3, 0, NCH, partner),
        (4, 5, 0, NCH, partner),
        (4, 6, 0, half, nbr_x),
        (2, 6, half, half, nbr_y),
        (6, 7, 0, NCH, partner),
    )

    def y_move(idx):
        src, dst, lo, n, dev = y_moves[idx]
        return y_copy(src, dst, lo, n, idx, dev)

    def y_arrived(idx):
        _, dst, lo, n, dev = y_moves[idx]
        return y_copy(dst, dst, lo, n, idx, dev)

    for idx in range(3):
        y_move(idx).start()

    for parity in range(2):
        written(parity)
    for number in range(RING):
        read_k(jnp.int32(number)).start()

    def second(t):
        s = 2 * t

        @pl.when(s == 12)
        def _():
            y_arrived(0).wait_recv()

        @pl.when(s == 22)
        def _():
            y_arrived(1).wait_recv()
            y_arrived(2).wait_recv()
            for idx in range(3, 7):
                y_move(idx).start()

        @pl.when(s == 28)
        def _():
            y_arrived(3).wait_recv()
            y_arrived(4).wait_recv()

        @pl.when(s == 56)
        def _():
            y_arrived(5).wait_recv()
            y_arrived(6).wait_recv()
            y_move(7).start()

        @pl.when(s == 70)
        def _():
            y_arrived(7).wait_recv()

        streamed, number, slot = stream_of(t)

        @pl.when(streamed)
        def _():
            read_k(number).wait()

        lhs = pair_of(yall, t)

        @pl.when(streamed)
        def _():
            for i in range(NCH):
                apply(stage, split(number, RING, 171, 512)[1], lhs, i)

        @pl.when(jnp.logical_not(streamed))
        def _():
            for i in range(NCH):
                apply(kept, slot, lhs, i)

        @pl.when(jnp.logical_and(streamed, number + RING < N_STREAM))
        def _():
            read_k(number + RING).start()

    @pl.loop(0, PAIRS)
    def _(t):
        second(t)

    for idx in range(8):
        y_move(idx).wait_send()

    @pl.loop(0, NCH)
    def _(k):
        out_ref[k] = ysum[k]


def solution(mesh):
    rows = NCH * T

    def local_program(x_loc, v_loc, length_scale, out_scale):
        vt_loc = v_loc.reshape(NCH, T, COLS).transpose(0, 2, 1)
        dma = pltpu.SemaphoreType.DMA
        out, _, _ = pl.pallas_call(
            body,
            out_shape=(
                jax.ShapeDtypeStruct((NCH, COLS, T), jnp.float32),
                jax.ShapeDtypeStruct((NREL, NCH, T, FEAT), jnp.bfloat16),
                jax.ShapeDtypeStruct((N_STREAM, NCH, 2, 2 * T, 128), jnp.bfloat16),
            ),
            in_specs=[
                pl.BlockSpec(memory_space=pltpu.HBM),
                pl.BlockSpec(memory_space=pltpu.HBM),
                pl.BlockSpec(memory_space=pltpu.SMEM),
                pl.BlockSpec(memory_space=pltpu.SMEM),
            ],
            out_specs=(
                pl.BlockSpec(memory_space=pltpu.VMEM),
                pl.BlockSpec(memory_space=pltpu.HBM),
                pl.BlockSpec(memory_space=pltpu.HBM),
            ),
            scratch_shapes=[
                pltpu.VMEM((NCH, 2, FEAT, 128), jnp.bfloat16),
                pltpu.VMEM((NREL, NCH, COLS, T), jnp.bfloat16),
                pltpu.VMEM((NREL, NCH, COLS, T), jnp.bfloat16),
                pltpu.VMEM((N_RES, NCH, 2, 2 * T, 128), jnp.bfloat16),
                pltpu.VMEM((RING, NCH, 2, 2 * T, 128), jnp.bfloat16),
                pltpu.VMEM((XR, 2 * T, FEAT), jnp.bfloat16),
                pltpu.VMEM((2 * T, 128), jnp.float32),
                pltpu.VMEM((NCH, 8, T), jnp.float32),
                dma((XR, 2)), dma((2,)), dma((RING,)), dma,
                dma((NREL, NCH)), dma((NREL, NCH)),
                dma((3, NCH)), dma((3, NCH)),
                dma((3, NCH)), dma((3, NCH)),
                dma((NCH,)), dma((NCH,)),
                dma((8,)), dma((8,)),
                pltpu.VMEM((NCH, COLS, T), jnp.float32),
                pltpu.VMEM((2, 8, 128), jnp.float32),
                dma((NCH,)),
            ],
            compiler_params=pltpu.CompilerParams(
                collective_id=0,
                has_side_effects=True,
                vmem_limit_bytes=67_043_328
            ),
        )(x_loc.reshape(NCH, T, FEAT), vt_loc, length_scale, out_scale)
        return out.transpose(0, 2, 1).reshape(rows, COLS)

    row_spec = P(("task", "row"), None)
    return jax.shard_map(
        local_program,
        mesh=mesh,
        in_specs=(row_spec, row_spec, P("task"), P("task")),
        out_specs=row_spec,
        check_vma=False,
    )
```

```python
import functools
import math

import jax
import jax.numpy as jnp
from jax import lax
from jax.experimental import pallas as pl
from jax.experimental.pallas import tpu as pltpu
from jax.sharding import PartitionSpec as P

MESH = pl.DeviceIdType.MESH
T = 256
FEAT = 512
COLS = 64
NCH = 12
NREL = 8
STEPS = NREL * NCH
PIECE = 64
NP = T // PIECE
NI = NCH // 2
PAIRS = STEPS // 2
RES_IN, RES_OF = 2, 5
N_RES = (PAIRS - 12) // RES_OF * RES_IN
RING = 3
N_STREAM = PAIRS - N_RES
XR = 2


def split(n, by, factor, power):
    whole = lax.div(n * factor, power)
    return whole, n - whole * by


def chunk_of(s):
    j = lax.rem(s + 2, 4)
    v = lax.div(s - 22, 4) - 1
    late = jnp.where(s < 26, 0, jnp.where(s >= 94, 1, lax.div(j, 2)))
    group = jnp.where(s < 26, 0, jnp.where(s >= 94, 17, v + 1 - late))
    side = lax.rem(s, 2)
    far = group >= 12
    rel = jnp.where(far, 6, 2 + 2 * side) + late
    chunk = jnp.where(far, 2 * (group - 12) + side, group)
    near_rel, near_chunk = split(s, NCH, 43, 512)
    return jnp.where(s < 24, near_rel, rel), jnp.where(s < 24, near_chunk, chunk)


def wide(left, right):
    return jnp.concatenate([left, right], axis=1)


def stream_of(t):
    u = jnp.maximum(t - 12, 0)
    o, w = split(u, RES_OF, 205, 1024)
    keep = jnp.where(o == (PAIRS - 12) // RES_OF, 0, RES_IN)
    streamed = jnp.logical_or(t < 12, w >= keep)
    number = jnp.where(t < 12, t, 12 + o * (RES_OF - RES_IN) + w - keep)
    return streamed, number, o * RES_IN + w


def body(
    x_hbm, vt_hbm, ls_ref, os_ref,
    out_ref, xall, kst,
    xt, vt, yall, kept, stage, xr, nj, ni,
    ld_sem, kw_sem, kr_sem, vl_sem,
    rx_sem, rv_sem, so_x, so_v, sp_x, sp_v, sn_x, sn_v, ys_sem, yr_sem,
    ysum, consts, su_sem,
):
    me = lax.axis_index("row")
    partner = me + 1 - 2 * lax.rem(me, 2)
    nbr_x = me + 2 - 4 * lax.rem(lax.div(me, 2), 2)
    nbr_y = me + 4 - 8 * lax.div(me, 4)

    def remote(src, dst, ss, rs, dev):
        return pltpu.make_async_remote_copy(
            src_ref=src, dst_ref=dst, send_sem=ss, recv_sem=rs, device_id={"row": dev}, device_id_type=MESH
        )

    def send_own(k, which, dev):
        slot = (1, 2, 4)[which]
        return (
            remote(x_hbm.at[k], xall.at[slot, k], so_x.at[which, k], rx_sem.at[slot, k], dev),
            remote(vt_hbm.at[k], vt.at[slot, k], so_v.at[which, k], rv_sem.at[slot, k], dev),
        )

    def forward_partner(rel, k):
        row = lax.div(rel, 2) - 1
        return (
            remote(xall.at[rel, k], xall.at[rel + 1, k], sp_x.at[row, k], rx_sem.at[rel + 1, k], partner),
            remote(vt.at[rel, k], vt.at[rel + 1, k], sp_v.at[row, k], rv_sem.at[rel + 1, k], partner),
        )

    def forward_nbr(rel, k, dev):
        return (
            remote(xall.at[rel, k], xall.at[6, k], sn_x.at[k], rx_sem.at[6, k], dev),
            remote(vt.at[rel, k], vt.at[6, k], sn_v.at[k], rv_sem.at[6, k], dev),
        )

    barrier = pltpu.get_barrier_semaphore()
    for dev in (partner, nbr_x, nbr_y):
        pl.semaphore_signal(barrier, inc=1, device_id={"row": dev}, device_id_type=MESH)

    own_v = pltpu.make_async_copy(vt_hbm, vt.at[0], vl_sem)
    own_v.start()

    def load_own(k, slot, half):
        return pltpu.make_async_copy(x_hbm.at[k], xr.at[slot, pl.ds(half * T, T)], ld_sem.at[slot, half])

    @pl.loop(0, NCH)
    def _(k):
        for q in range(4):
            pltpu.make_async_copy(
                x_hbm.at[k, :, pl.ds(q * 128, 128)],
                stage.at[RING - 1, k, q // 2, pl.ds(q % 2 * T, T)],
                su_sem.at[k],
            ).start()

    load_own(0, 0, 0).start()
    load_own(1, 0, 1).start()
    pl.semaphore_wait(barrier, 3)

    @pl.loop(0, NCH)
    def _(k):
        for which, dev in enumerate((partner, nbr_x, nbr_y)):
            for copy in send_own(k, which, dev):
                copy.start()

    @pl.loop(0, NCH)
    def _(k):
        pltpu.make_async_copy(x_hbm.at[k], xr.at[1, pl.ds(0, T)], su_sem.at[k]).wait()
        norm = jnp.zeros((1, T), jnp.float32)
        for q in range(4):
            part = stage[RING - 1, k, q // 2, q % 2 * T : (q % 2 + 1) * T, :].astype(jnp.float32).T
            norm = norm + jnp.sum(part * part, axis=0, keepdims=True)
            scaled = (part * -2.0).astype(jnp.bfloat16)
            for side in range(2):
                xt[k, side, q * 128 : (q + 1) * 128, :] = scaled[:, side * 128 : (side + 1) * 128]
        ni[k] = jnp.broadcast_to(norm, (8, T))

    own_v.wait()

    scale = jnp.full((8, 128), ls_ref[0], jnp.float32)
    consts[0] = -math.log2(math.e) / (2.0 * scale * scale)
    consts[1] = jnp.full((8, 128), os_ref[0], jnp.float32)

    @pl.loop(0, NCH)
    def _(k):
        ysum[k] = jnp.zeros((COLS, T), jnp.float32)

    def write_k(t, parity):
        streamed, number, slot = stream_of(t)

        @pl.when(streamed)
        def _():
            pltpu.make_async_copy(stage.at[parity], kst.at[number], kw_sem.at[parity]).start()

        @pl.when(jnp.logical_not(streamed))
        def _():
            pltpu.make_async_copy(stage.at[parity], kept.at[slot], kw_sem.at[parity]).start()

    def written(parity):
        pltpu.make_async_copy(stage.at[parity], kst.at[0], kw_sem.at[parity]).wait()

    def read_k(number, slot):
        return pltpu.make_async_copy(kst.at[number], stage.at[slot], kr_sem.at[slot])

    def weigh(x_slot, parity, i):
        gram_tile = jnp.dot(xr[x_slot], wide(xt[i, 0], xt[i, 1]), preferred_element_type=jnp.float32)
        for h in range(2):
            lanes = slice(h * 128, (h + 1) * 128)
            dist = jnp.maximum((nj[...] + ni[i, 0:1, lanes]) + gram_tile[:, lanes], 0.0)
            stage[parity, i, h] = (consts[1, 0:1, :] * jnp.exp2(dist * consts[0, 0:1, :])).astype(jnp.bfloat16)

    def apply(source, slot, lhs, i):
        ysum[i] += jnp.dot(lhs, wide(source[slot, i, 0], source[slot, i, 1]), preferred_element_type=jnp.float32)

    def pair_of(table, t):
        rel, k = chunk_of(2 * t)
        rel_2, k_2 = chunk_of(2 * t + 1)
        return jnp.concatenate([table[rel, k], table[rel_2, k_2]], axis=1)

    def fetch(s):
        rel, k = chunk_of(s)
        half = lax.rem(s, 2)
        slot = lax.rem(lax.div(s, 2), XR)

        @pl.when(rel == 0)
        def _():
            load_own(k, slot, half).start()

        @pl.when(rel > 0)
        def _():
            remote(xall.at[rel, k], xall.at[rel, k], so_x.at[0, 0], rx_sem.at[rel, k], partner).wait_recv()
            remote(vt.at[rel, k], vt.at[rel, k], so_v.at[0, 0], rv_sem.at[rel, k], partner).wait_recv()
            pltpu.make_async_copy(
                xall.at[rel, k], xr.at[slot, pl.ds(half * T, T)], ld_sem.at[slot, half]
            ).start()

        @pl.when(jnp.logical_and(rel >= 2, lax.rem(rel, 2) == 0))
        def _():
            for copy in forward_partner(rel, k):
                copy.start()

        @pl.when(jnp.logical_and(rel == 2, lax.rem(k, 2) == 1))
        def _():
            for copy in forward_nbr(2, k, nbr_y):
                copy.start()

        @pl.when(jnp.logical_and(rel == 4, lax.rem(k, 2) == 0))
        def _():
            for copy in forward_nbr(4, k, nbr_x):
                copy.start()

    def trip(t, parity, place):
        if place < 2:
            fetch(2 * t + 2)
            fetch(2 * t + 3)
        if place > 0:
            write_k(t - 1, 1 - parity)

            @pl.when(t >= 2)
            def _():
                written(parity)

        x_slot = parity
        load_own(0, x_slot, 0).wait()
        load_own(0, x_slot, 1).wait()
        for p in range(2 * NP):
            rows = slice(p * PIECE, (p + 1) * PIECE)
            part = xr[x_slot, rows, :].astype(jnp.float32)
            norm = jnp.sum(part * part, axis=1, keepdims=True)
            nj[rows, :] = jnp.broadcast_to(norm, (PIECE, 128))
        if place > 0:
            lhs = pair_of(vt, t - 1)
        for i in range(NCH + 6):
            if place > 0 and i >= 6:
                apply(stage, 1 - parity, lhs, i - 6)
            if i < NCH:
                weigh(x_slot, parity, i)

    trip(jnp.int32(0), 0, 0)

    @pl.loop(0, PAIRS // 2 - 1)
    def _(m):
        trip(2 * m + 1, 1, 1)
        trip(2 * m + 2, 0, 1)

    trip(jnp.int32(PAIRS - 1), 1, 2)
    write_k(jnp.int32(PAIRS - 1), 1)
    lhs = pair_of(vt, jnp.int32(PAIRS - 1))
    for i in range(NCH):
        apply(stage, 1, lhs, i)

    @pl.loop(0, NCH)
    def _(k):
        yall[0, k] = ysum[k].astype(jnp.bfloat16)
        ysum[k] = jnp.zeros((COLS, T), jnp.float32)

    @pl.loop(0, NCH)
    def _(k):
        for which, dev in enumerate((partner, nbr_x, nbr_y)):
            for copy in send_own(k, which, dev):
                copy.wait_send()
        for rel in (2, 4, 6):
            for copy in forward_partner(rel, k):
                copy.wait_send()
        for copy in forward_nbr(2, k, nbr_y):
            copy.wait_send()

    half = NCH // 2

    def y_copy(src_rel, dst_rel, lo, n, idx, dev):
        return remote(
            yall.at[src_rel, pl.ds(lo, n)], yall.at[dst_rel, pl.ds(lo, n)], ys_sem.at[idx], yr_sem.at[idx], dev
        )

    y_moves = (
        (0, 1, 0, NCH, partner),
        (0, 2, 0, NCH, nbr_x),
        (0, 4, 0, NCH, nbr_y),
        (2, 3, 0, NCH, partner),
        (4, 5, 0, NCH, partner),
        (4, 6, 0, half, nbr_x),
        (2, 6, half, half, nbr_y),
        (6, 7, 0, NCH, partner),
    )

    def y_move(idx):
        src, dst, lo, n, dev = y_moves[idx]
        return y_copy(src, dst, lo, n, idx, dev)

    def y_arrived(idx):
        _, dst, lo, n, dev = y_moves[idx]
        return y_copy(dst, dst, lo, n, idx, dev)

    for idx in range(3):
        y_move(idx).start()

    for parity in range(2):
        written(parity)
    for number in range(RING):
        read_k(jnp.int32(number), number).start()

    def use(t, source, slot):
        lhs = pair_of(yall, t)
        for i in range(NCH):
            apply(source, slot, lhs, i)

    def use_streamed(t, number, slot):
        read_k(number, slot).wait()
        use(t, stage, slot)

        @pl.when(number + RING < N_STREAM)
        def _():
            read_k(number + RING, slot).start()

    def use_first(lo, hi):
        @pl.loop(lo, hi)
        def _(m):
            @pl.when(m == 2)
            def _():
                y_arrived(0).wait_recv()

            for slot in range(RING):
                use_streamed(RING * m + slot, RING * m + slot, slot)

    use_first(0, 3)
    y_arrived(1).wait_recv()
    y_arrived(2).wait_recv()
    for idx in range(3, 7):
        y_move(idx).start()
    use_first(3, 4)
    y_arrived(3).wait_recv()
    y_arrived(4).wait_recv()

    @pl.loop(0, (PAIRS - 12) // RES_OF)
    def _(o):
        @pl.when(o == 3)
        def _():
            y_arrived(5).wait_recv()
            y_arrived(6).wait_recv()
            y_move(7).start()

        @pl.when(o == 5)
        def _():
            y_arrived(7).wait_recv()

        t = 12 + o * RES_OF
        for slot in range(RING):
            use_streamed(t + RES_IN + slot, 12 + o * RING + slot, slot)
            if slot < RES_IN:
                use(t + slot, kept, o * RES_IN + slot)

    use_streamed(jnp.int32(PAIRS - 1), jnp.int32(N_STREAM - 1), 0)

    for idx in range(8):
        y_move(idx).wait_send()

    @pl.loop(0, NCH)
    def _(k):
        out_ref[k] = ysum[k]


def solution(mesh):
    rows = NCH * T

    def local_program(x_loc, v_loc, length_scale, out_scale):
        vt_loc = v_loc.reshape(NCH, T, COLS).transpose(0, 2, 1)
        dma = pltpu.SemaphoreType.DMA
        out, _, _ = pl.pallas_call(
            body,
            out_shape=(
                jax.ShapeDtypeStruct((NCH, COLS, T), jnp.float32),
                jax.ShapeDtypeStruct((NREL, NCH, T, FEAT), jnp.bfloat16),
                jax.ShapeDtypeStruct((N_STREAM, NCH, 2, 2 * T, 128), jnp.bfloat16),
            ),
            in_specs=[
                pl.BlockSpec(memory_space=pltpu.HBM),
                pl.BlockSpec(memory_space=pltpu.HBM),
                pl.BlockSpec(memory_space=pltpu.SMEM),
                pl.BlockSpec(memory_space=pltpu.SMEM),
            ],
            out_specs=(
                pl.BlockSpec(memory_space=pltpu.VMEM),
                pl.BlockSpec(memory_space=pltpu.HBM),
                pl.BlockSpec(memory_space=pltpu.HBM),
            ),
            scratch_shapes=[
                pltpu.VMEM((NCH, 2, FEAT, 128), jnp.bfloat16),
                pltpu.VMEM((NREL, NCH, COLS, T), jnp.bfloat16),
                pltpu.VMEM((NREL, NCH, COLS, T), jnp.bfloat16),
                pltpu.VMEM((N_RES, NCH, 2, 2 * T, 128), jnp.bfloat16),
                pltpu.VMEM((RING, NCH, 2, 2 * T, 128), jnp.bfloat16),
                pltpu.VMEM((XR, 2 * T, FEAT), jnp.bfloat16),
                pltpu.VMEM((2 * T, 128), jnp.float32),
                pltpu.VMEM((NCH, 8, T), jnp.float32),
                dma((XR, 2)), dma((2,)), dma((RING,)), dma,
                dma((NREL, NCH)), dma((NREL, NCH)),
                dma((3, NCH)), dma((3, NCH)),
                dma((3, NCH)), dma((3, NCH)),
                dma((NCH,)), dma((NCH,)),
                dma((8,)), dma((8,)),
                pltpu.VMEM((NCH, COLS, T), jnp.float32),
                pltpu.VMEM((2, 8, 128), jnp.float32),
                dma((NCH,)),
            ],
            compiler_params=pltpu.CompilerParams(
                collective_id=0,
                has_side_effects=True,
                vmem_limit_bytes=67_043_328
            ),
        )(x_loc.reshape(NCH, T, FEAT), vt_loc, length_scale, out_scale)
        return out.transpose(0, 2, 1).reshape(rows, COLS)

    row_spec = P(("task", "row"), None)
    return jax.shard_map(
        local_program,
        mesh=mesh,
        in_specs=(row_spec, row_spec, P("task"), P("task")),
        out_specs=row_spec,
        check_vma=False,
    )
```

```python
import functools
import math

import jax
import jax.numpy as jnp
from jax import lax
from jax.experimental import pallas as pl
from jax.experimental.pallas import tpu as pltpu
from jax.sharding import PartitionSpec as P

MESH = pl.DeviceIdType.MESH
T = 256
FEAT = 512
COLS = 64
NCH = 12
NREL = 8
STEPS = NREL * NCH
PIECE = 64
NP = T // PIECE
NI = NCH // 2
PAIRS = STEPS // 2
RES_IN, RES_OF = 2, 5
N_RES = (PAIRS - 12) // RES_OF * RES_IN
RING = 3
N_STREAM = PAIRS - N_RES
XR = 2


def split(n, by, factor, power):
    whole = lax.div(n * factor, power)
    return whole, n - whole * by


def chunk_of(s):
    j = lax.rem(s + 2, 4)
    v = lax.div(s - 22, 4) - 1
    late = jnp.where(s < 26, 0, jnp.where(s >= 94, 1, lax.div(j, 2)))
    group = jnp.where(s < 26, 0, jnp.where(s >= 94, 17, v + 1 - late))
    side = lax.rem(s, 2)
    far = group >= 12
    rel = jnp.where(far, 6, 2 + 2 * side) + late
    chunk = jnp.where(far, 2 * (group - 12) + side, group)
    near_rel, near_chunk = split(s, NCH, 43, 512)
    return jnp.where(s < 24, near_rel, rel), jnp.where(s < 24, near_chunk, chunk)


def wide(left, right):
    return jnp.concatenate([left, right], axis=1)


def stream_of(t):
    u = jnp.maximum(t - 12, 0)
    o, w = split(u, RES_OF, 205, 1024)
    keep = jnp.where(o == (PAIRS - 12) // RES_OF, 0, RES_IN)
    streamed = jnp.logical_or(t < 12, w >= keep)
    number = jnp.where(t < 12, t, 12 + o * (RES_OF - RES_IN) + w - keep)
    return streamed, number, o * RES_IN + w


def body(
    x_hbm, vt_hbm, ls_ref, os_ref,
    out_ref, xall, kst,
    xt, vt, yall, kept, stage, xr, nj, ni,
    ld_sem, kw_sem, kr_sem, vl_sem,
    rx_sem, rv_sem, so_x, so_v, sp_x, sp_v, sn_x, sn_v, ys_sem, yr_sem,
    ysum, consts, su_sem,
):
    me = lax.axis_index("row")
    partner = me + 1 - 2 * lax.rem(me, 2)
    nbr_x = me + 2 - 4 * lax.rem(lax.div(me, 2), 2)
    nbr_y = me + 4 - 8 * lax.div(me, 4)

    def remote(src, dst, ss, rs, dev):
        return pltpu.make_async_remote_copy(
            src_ref=src, dst_ref=dst, send_sem=ss, recv_sem=rs, device_id={"row": dev}, device_id_type=MESH
        )

    def send_own(k, which, dev):
        slot = (1, 2, 4)[which]
        return (
            remote(x_hbm.at[k], xall.at[slot, k], so_x.at[which, k], rx_sem.at[slot, k], dev),
            remote(vt_hbm.at[k], vt.at[slot, k], so_v.at[which, k], rv_sem.at[slot, k], dev),
        )

    def forward_partner(rel, k):
        row = lax.div(rel, 2) - 1
        return (
            remote(xall.at[rel, k], xall.at[rel + 1, k], sp_x.at[row, k], rx_sem.at[rel + 1, k], partner),
            remote(vt.at[rel, k], vt.at[rel + 1, k], sp_v.at[row, k], rv_sem.at[rel + 1, k], partner),
        )

    def forward_nbr(rel, k, dev):
        return (
            remote(xall.at[rel, k], xall.at[6, k], sn_x.at[k], rx_sem.at[6, k], dev),
            remote(vt.at[rel, k], vt.at[6, k], sn_v.at[k], rv_sem.at[6, k], dev),
        )

    barrier = pltpu.get_barrier_semaphore()
    for dev in (partner, nbr_x, nbr_y):
        pl.semaphore_signal(barrier, inc=1, device_id={"row": dev}, device_id_type=MESH)

    own_v = pltpu.make_async_copy(vt_hbm, vt.at[0], vl_sem)
    own_v.start()

    def load_own(k, slot, half):
        return pltpu.make_async_copy(x_hbm.at[k], xr.at[slot, pl.ds(half * T, T)], ld_sem.at[slot, half])

    @pl.loop(0, NCH)
    def _(k):
        for q in range(4):
            pltpu.make_async_copy(
                x_hbm.at[k, :, pl.ds(q * 128, 128)],
                stage.at[RING - 1, k, q // 2, pl.ds(q % 2 * T, T)],
                su_sem.at[k],
            ).start()

    load_own(0, 0, 0).start()
    load_own(1, 0, 1).start()
    pl.semaphore_wait(barrier, 3)

    @pl.loop(0, NCH)
    def _(k):
        for which, dev in enumerate((partner, nbr_x, nbr_y)):
            for copy in send_own(k, which, dev):
                copy.start()

    @pl.loop(0, NCH)
    def _(k):
        pltpu.make_async_copy(x_hbm.at[k], xr.at[1, pl.ds(0, T)], su_sem.at[k]).wait()
        norm = jnp.zeros((1, T), jnp.float32)
        for q in range(4):
            part = stage[RING - 1, k, q // 2, q % 2 * T : (q % 2 + 1) * T, :].astype(jnp.float32).T
            norm = norm + jnp.sum(part * part, axis=0, keepdims=True)
            scaled = (part * -2.0).astype(jnp.bfloat16)
            for side in range(2):
                xt[k, side, q * 128 : (q + 1) * 128, :] = scaled[:, side * 128 : (side + 1) * 128]
        ni[k] = jnp.broadcast_to(norm, (8, T))

    own_v.wait()

    scale = jnp.full((8, 128), ls_ref[0], jnp.float32)
    consts[0] = -math.log2(math.e) / (2.0 * scale * scale)
    consts[1] = jnp.full((8, 128), os_ref[0], jnp.float32)

    @pl.loop(0, NCH)
    def _(k):
        ysum[k] = jnp.zeros((COLS, T), jnp.float32)

    def write_k(t, parity):
        streamed, number, slot = stream_of(t)

        @pl.when(streamed)
        def _():
            pltpu.make_async_copy(stage.at[parity], kst.at[number], kw_sem.at[parity]).start()

        @pl.when(jnp.logical_not(streamed))
        def _():
            pltpu.make_async_copy(stage.at[parity], kept.at[slot], kw_sem.at[parity]).start()

    def written(parity):
        pltpu.make_async_copy(stage.at[parity], kst.at[0], kw_sem.at[parity]).wait()

    def read_k(number, slot):
        return pltpu.make_async_copy(kst.at[number], stage.at[slot], kr_sem.at[slot])

    def weigh(x_slot, parity, i):
        if i % 2:
            return
        both = wide(wide(xt[i, 0], xt[i, 1]), wide(xt[i + 1, 0], xt[i + 1, 1]))
        for c in range(2):
            rows = slice(c * 256, (c + 1) * 256)
            tiles = jnp.dot(xr[x_slot, rows, :], both, preferred_element_type=jnp.float32)
            finish(tiles[:, :T], parity, i, rows)
            finish(tiles[:, T:], parity, i + 1, rows)

    def finish(gram_tile, parity, i, rows):
        for h in range(2):
            lanes = slice(h * 128, (h + 1) * 128)
            dist = jnp.maximum((nj[rows, :] + ni[i, 0:1, lanes]) + gram_tile[:, lanes], 0.0)
            stage[parity, i, h, rows] = (consts[1, 0:1, :] * jnp.exp2(dist * consts[0, 0:1, :])).astype(jnp.bfloat16)

    def apply(source, slot, lhs, i):
        ysum[i] += jnp.dot(lhs, wide(source[slot, i, 0], source[slot, i, 1]), preferred_element_type=jnp.float32)

    def pair_of(table, t):
        rel, k = chunk_of(2 * t)
        rel_2, k_2 = chunk_of(2 * t + 1)
        return jnp.concatenate([table[rel, k], table[rel_2, k_2]], axis=1)

    def fetch(s):
        rel, k = chunk_of(s)
        half = lax.rem(s, 2)
        slot = lax.rem(lax.div(s, 2), XR)

        @pl.when(rel == 0)
        def _():
            load_own(k, slot, half).start()

        @pl.when(rel > 0)
        def _():
            remote(xall.at[rel, k], xall.at[rel, k], so_x.at[0, 0], rx_sem.at[rel, k], partner).wait_recv()
            remote(vt.at[rel, k], vt.at[rel, k], so_v.at[0, 0], rv_sem.at[rel, k], partner).wait_recv()
            pltpu.make_async_copy(
                xall.at[rel, k], xr.at[slot, pl.ds(half * T, T)], ld_sem.at[slot, half]
            ).start()

        @pl.when(jnp.logical_and(rel >= 2, lax.rem(rel, 2) == 0))
        def _():
            for copy in forward_partner(rel, k):
                copy.start()

        @pl.when(jnp.logical_and(rel == 2, lax.rem(k, 2) == 1))
        def _():
            for copy in forward_nbr(2, k, nbr_y):
                copy.start()

        @pl.when(jnp.logical_and(rel == 4, lax.rem(k, 2) == 0))
        def _():
            for copy in forward_nbr(4, k, nbr_x):
                copy.start()

    def trip(t, parity, place):
        if place < 2:
            fetch(2 * t + 2)
            fetch(2 * t + 3)
        if place > 0:
            write_k(t - 1, 1 - parity)

            @pl.when(t >= 2)
            def _():
                written(parity)

        x_slot = parity
        load_own(0, x_slot, 0).wait()
        load_own(0, x_slot, 1).wait()
        for p in range(2 * NP):
            rows = slice(p * PIECE, (p + 1) * PIECE)
            part = xr[x_slot, rows, :].astype(jnp.float32)
            norm = jnp.sum(part * part, axis=1, keepdims=True)
            nj[rows, :] = jnp.broadcast_to(norm, (PIECE, 128))
        if place > 0:
            lhs = pair_of(vt, t - 1)
        for i in range(NCH + 6):
            if place > 0 and i >= 6:
                apply(stage, 1 - parity, lhs, i - 6)
            if i < NCH:
                weigh(x_slot, parity, i)

    trip(jnp.int32(0), 0, 0)

    @pl.loop(0, PAIRS // 2 - 1)
    def _(m):
        trip(2 * m + 1, 1, 1)
        trip(2 * m + 2, 0, 1)

    trip(jnp.int32(PAIRS - 1), 1, 2)
    write_k(jnp.int32(PAIRS - 1), 1)
    lhs = pair_of(vt, jnp.int32(PAIRS - 1))
    for i in range(NCH):
        apply(stage, 1, lhs, i)

    @pl.loop(0, NCH)
    def _(k):
        yall[0, k] = ysum[k].astype(jnp.bfloat16)
        ysum[k] = jnp.zeros((COLS, T), jnp.float32)

    @pl.loop(0, NCH)
    def _(k):
        for which, dev in enumerate((partner, nbr_x, nbr_y)):
            for copy in send_own(k, which, dev):
                copy.wait_send()
        for rel in (2, 4, 6):
            for copy in forward_partner(rel, k):
                copy.wait_send()
        for copy in forward_nbr(2, k, nbr_y):
            copy.wait_send()

    half = NCH // 2

    def y_copy(src_rel, dst_rel, lo, n, idx, dev):
        return remote(
            yall.at[src_rel, pl.ds(lo, n)], yall.at[dst_rel, pl.ds(lo, n)], ys_sem.at[idx], yr_sem.at[idx], dev
        )

    y_moves = (
        (0, 1, 0, NCH, partner),
        (0, 2, 0, NCH, nbr_x),
        (0, 4, 0, NCH, nbr_y),
        (2, 3, 0, NCH, partner),
        (4, 5, 0, NCH, partner),
        (4, 6, 0, half, nbr_x),
        (2, 6, half, half, nbr_y),
        (6, 7, 0, NCH, partner),
    )

    def y_move(idx):
        src, dst, lo, n, dev = y_moves[idx]
        return y_copy(src, dst, lo, n, idx, dev)

    def y_arrived(idx):
        _, dst, lo, n, dev = y_moves[idx]
        return y_copy(dst, dst, lo, n, idx, dev)

    for idx in range(3):
        y_move(idx).start()

    for parity in range(2):
        written(parity)
    for number in range(RING):
        read_k(jnp.int32(number), number).start()

    def use(t, source, slot):
        lhs = pair_of(yall, t)
        for i in range(NCH):
            apply(source, slot, lhs, i)

    def use_streamed(t, number, slot):
        read_k(number, slot).wait()
        use(t, stage, slot)

        @pl.when(number + RING < N_STREAM)
        def _():
            read_k(number + RING, slot).start()

    def use_first(lo, hi):
        @pl.loop(lo, hi)
        def _(m):
            @pl.when(m == 2)
            def _():
                y_arrived(0).wait_recv()

            for slot in range(RING):
                use_streamed(RING * m + slot, RING * m + slot, slot)

    use_first(0, 3)
    y_arrived(1).wait_recv()
    y_arrived(2).wait_recv()
    for idx in range(3, 7):
        y_move(idx).start()
    use_first(3, 4)
    y_arrived(3).wait_recv()
    y_arrived(4).wait_recv()

    @pl.loop(0, (PAIRS - 12) // RES_OF)
    def _(o):
        @pl.when(o == 3)
        def _():
            y_arrived(5).wait_recv()
            y_arrived(6).wait_recv()
            y_move(7).start()

        @pl.when(o == 5)
        def _():
            y_arrived(7).wait_recv()

        t = 12 + o * RES_OF
        for slot in range(RING):
            use_streamed(t + RES_IN + slot, 12 + o * RING + slot, slot)
            if slot < RES_IN:
                use(t + slot, kept, o * RES_IN + slot)

    use_streamed(jnp.int32(PAIRS - 1), jnp.int32(N_STREAM - 1), 0)

    for idx in range(8):
        y_move(idx).wait_send()

    @pl.loop(0, NCH)
    def _(k):
        out_ref[k] = ysum[k]


def solution(mesh):
    rows = NCH * T

    def local_program(x_loc, v_loc, length_scale, out_scale):
        vt_loc = v_loc.reshape(NCH, T, COLS).transpose(0, 2, 1)
        dma = pltpu.SemaphoreType.DMA
        out, _, _ = pl.pallas_call(
            body,
            out_shape=(
                jax.ShapeDtypeStruct((NCH, COLS, T), jnp.float32),
                jax.ShapeDtypeStruct((NREL, NCH, T, FEAT), jnp.bfloat16),
                jax.ShapeDtypeStruct((N_STREAM, NCH, 2, 2 * T, 128), jnp.bfloat16),
            ),
            in_specs=[
                pl.BlockSpec(memory_space=pltpu.HBM),
                pl.BlockSpec(memory_space=pltpu.HBM),
                pl.BlockSpec(memory_space=pltpu.SMEM),
                pl.BlockSpec(memory_space=pltpu.SMEM),
            ],
            out_specs=(
                pl.BlockSpec(memory_space=pltpu.VMEM),
                pl.BlockSpec(memory_space=pltpu.HBM),
                pl.BlockSpec(memory_space=pltpu.HBM),
            ),
            scratch_shapes=[
                pltpu.VMEM((NCH, 2, FEAT, 128), jnp.bfloat16),
                pltpu.VMEM((NREL, NCH, COLS, T), jnp.bfloat16),
                pltpu.VMEM((NREL, NCH, COLS, T), jnp.bfloat16),
                pltpu.VMEM((N_RES, NCH, 2, 2 * T, 128), jnp.bfloat16),
                pltpu.VMEM((RING, NCH, 2, 2 * T, 128), jnp.bfloat16),
                pltpu.VMEM((XR, 2 * T, FEAT), jnp.bfloat16),
                pltpu.VMEM((2 * T, 128), jnp.float32),
                pltpu.VMEM((NCH, 8, T), jnp.float32),
                dma((XR, 2)), dma((2,)), dma((RING,)), dma,
                dma((NREL, NCH)), dma((NREL, NCH)),
                dma((3, NCH)), dma((3, NCH)),
                dma((3, NCH)), dma((3, NCH)),
                dma((NCH,)), dma((NCH,)),
                dma((8,)), dma((8,)),
                pltpu.VMEM((NCH, COLS, T), jnp.float32),
                pltpu.VMEM((2, 8, 128), jnp.float32),
                dma((NCH,)),
            ],
            compiler_params=pltpu.CompilerParams(
                collective_id=0,
                has_side_effects=True,
                vmem_limit_bytes=67_043_328
            ),
        )(x_loc.reshape(NCH, T, FEAT), vt_loc, length_scale, out_scale)
        return out.transpose(0, 2, 1).reshape(rows, COLS)

    row_spec = P(("task", "row"), None)
    return jax.shard_map(
        local_program,
        mesh=mesh,
        in_specs=(row_spec, row_spec, P("task"), P("task")),
        out_specs=row_spec,
        check_vma=False,
    )
```

```python
import functools
import math

import jax
import jax.numpy as jnp
from jax import lax
from jax.experimental import pallas as pl
from jax.experimental.pallas import tpu as pltpu
from jax.sharding import PartitionSpec as P

MESH = pl.DeviceIdType.MESH
T = 256
FEAT = 512
COLS = 64
NCH = 12
NREL = 8
STEPS = NREL * NCH
PIECE = 64
NP = T // PIECE
NI = NCH // 2
PAIRS = STEPS // 2
RES_IN, RES_OF = 2, 5
N_RES = (PAIRS - 12) // RES_OF * RES_IN
RING = 3
N_STREAM = PAIRS - N_RES
XR = 2


def split(n, by, factor, power):
    whole = lax.div(n * factor, power)
    return whole, n - whole * by


def chunk_of(s):
    j = lax.rem(s + 2, 4)
    v = lax.div(s - 22, 4) - 1
    late = jnp.where(s < 26, 0, jnp.where(s >= 94, 1, lax.div(j, 2)))
    group = jnp.where(s < 26, 0, jnp.where(s >= 94, 17, v + 1 - late))
    side = lax.rem(s, 2)
    far = group >= 12
    rel = jnp.where(far, 6, 2 + 2 * side) + late
    chunk = jnp.where(far, 2 * (group - 12) + side, group)
    near_rel, near_chunk = split(s, NCH, 43, 512)
    return jnp.where(s < 24, near_rel, rel), jnp.where(s < 24, near_chunk, chunk)


def wide(left, right):
    return jnp.concatenate([left, right], axis=1)


def stream_of(t):
    u = jnp.maximum(t - 12, 0)
    o, w = split(u, RES_OF, 205, 1024)
    keep = jnp.where(o == (PAIRS - 12) // RES_OF, 0, RES_IN)
    streamed = jnp.logical_or(t < 12, w >= keep)
    number = jnp.where(t < 12, t, 12 + o * (RES_OF - RES_IN) + w - keep)
    return streamed, number, o * RES_IN + w


def body(
    x_hbm, vt_hbm, ls_ref, os_ref,
    out_ref, xall, kst,
    xt, vt, yall, kept, stage, xr, nj, ni,
    ld_sem, kw_sem, kr_sem, vl_sem,
    rx_sem, rv_sem, so_x, so_v, sp_x, sp_v, sn_x, sn_v, ys_sem, yr_sem,
    ysum, consts, su_sem,
):
    me = lax.axis_index("row")
    partner = me + 1 - 2 * lax.rem(me, 2)
    nbr_x = me + 2 - 4 * lax.rem(lax.div(me, 2), 2)
    nbr_y = me + 4 - 8 * lax.div(me, 4)

    def remote(src, dst, ss, rs, dev):
        return pltpu.make_async_remote_copy(
            src_ref=src, dst_ref=dst, send_sem=ss, recv_sem=rs, device_id={"row": dev}, device_id_type=MESH
        )

    def send_own(k, which, dev):
        slot = (1, 2, 4)[which]
        return (
            remote(x_hbm.at[k], xall.at[slot, k], so_x.at[which, k], rx_sem.at[slot, k], dev),
            remote(vt_hbm.at[k], vt.at[slot, k], so_v.at[which, k], rv_sem.at[slot, k], dev),
        )

    def forward_partner(rel, k):
        row = lax.div(rel, 2) - 1
        return (
            remote(xall.at[rel, k], xall.at[rel + 1, k], sp_x.at[row, k], rx_sem.at[rel + 1, k], partner),
            remote(vt.at[rel, k], vt.at[rel + 1, k], sp_v.at[row, k], rv_sem.at[rel + 1, k], partner),
        )

    def forward_nbr(rel, k, dev):
        return (
            remote(xall.at[rel, k], xall.at[6, k], sn_x.at[k], rx_sem.at[6, k], dev),
            remote(vt.at[rel, k], vt.at[6, k], sn_v.at[k], rv_sem.at[6, k], dev),
        )

    barrier = pltpu.get_barrier_semaphore()
    for dev in (partner, nbr_x, nbr_y):
        pl.semaphore_signal(barrier, inc=1, device_id={"row": dev}, device_id_type=MESH)

    own_v = pltpu.make_async_copy(vt_hbm, vt.at[0], vl_sem)
    own_v.start()

    def load_own(k, slot, half):
        return pltpu.make_async_copy(x_hbm.at[k], xr.at[slot, pl.ds(half * T, T)], ld_sem.at[slot, half])

    @pl.loop(0, NCH)
    def _(k):
        for q in range(4):
            pltpu.make_async_copy(
                x_hbm.at[k, :, pl.ds(q * 128, 128)],
                stage.at[RING - 1, k, q // 2, pl.ds(q % 2 * T, T)],
                su_sem.at[k],
            ).start()

    load_own(0, 0, 0).start()
    load_own(1, 0, 1).start()
    pl.semaphore_wait(barrier, 3)

    @pl.loop(0, NCH)
    def _(k):
        for which, dev in enumerate((partner, nbr_x, nbr_y)):
            for copy in send_own(k, which, dev):
                copy.start()

    @pl.loop(0, NCH)
    def _(k):
        pltpu.make_async_copy(x_hbm.at[k], xr.at[1, pl.ds(0, T)], su_sem.at[k]).wait()
        norm = jnp.zeros((1, T), jnp.float32)
        for q in range(4):
            part = stage[RING - 1, k, q // 2, q % 2 * T : (q % 2 + 1) * T, :].astype(jnp.float32).T
            norm = norm + jnp.sum(part * part, axis=0, keepdims=True)
            scaled = (part * -2.0).astype(jnp.bfloat16)
            for side in range(2):
                xt[k, side, q * 128 : (q + 1) * 128, :] = scaled[:, side * 128 : (side + 1) * 128]
        ni[k] = jnp.broadcast_to(norm, (8, T))

    own_v.wait()

    scale = jnp.full((8, 128), ls_ref[0], jnp.float32)
    consts[0] = -math.log2(math.e) / (2.0 * scale * scale)
    consts[1] = jnp.full((8, 128), os_ref[0], jnp.float32)

    @pl.loop(0, NCH)
    def _(k):
        ysum[k] = jnp.zeros((COLS, T), jnp.float32)

    def write_k(t, parity):
        streamed, number, slot = stream_of(t)

        @pl.when(streamed)
        def _():
            pltpu.make_async_copy(stage.at[parity], kst.at[number], kw_sem.at[parity]).start()

        @pl.when(jnp.logical_not(streamed))
        def _():
            pltpu.make_async_copy(stage.at[parity], kept.at[slot], kw_sem.at[parity]).start()

    def written(parity):
        pltpu.make_async_copy(stage.at[parity], kst.at[0], kw_sem.at[parity]).wait()

    def read_k(number, slot):
        return pltpu.make_async_copy(kst.at[number], stage.at[slot], kr_sem.at[slot])

    def weigh(x_slot, parity, i):
        if i % 2:
            return
        both = wide(wide(xt[i, 0], xt[i, 1]), wide(xt[i + 1, 0], xt[i + 1, 1]))
        for c in range(2):
            rows = slice(c * 256, (c + 1) * 256)
            tiles = jnp.dot(xr[x_slot, rows, :], both, preferred_element_type=jnp.float32)
            finish(tiles[:, :T], parity, i, rows)
            finish(tiles[:, T:], parity, i + 1, rows)

    def finish(gram_tile, parity, i, rows):
        for h in range(2):
            lanes = slice(h * 128, (h + 1) * 128)
            dist = jnp.maximum((nj[rows, :] + ni[i, 0:1, lanes]) + gram_tile[:, lanes], 0.0)
            stage[parity, i, h, rows] = (consts[1, 0:1, :] * jnp.exp2(dist * consts[0, 0:1, :])).astype(jnp.bfloat16)

    def apply(source, slot, lhs, i):
        ysum[i] += jnp.dot(lhs, wide(source[slot, i, 0], source[slot, i, 1]), preferred_element_type=jnp.float32)

    def pair_of(table, t):
        rel, k = chunk_of(2 * t)
        rel_2, k_2 = chunk_of(2 * t + 1)
        return jnp.concatenate([table[rel, k], table[rel_2, k_2]], axis=1)

    def fetch(s):
        rel, k = chunk_of(s)
        half = lax.rem(s, 2)
        slot = lax.rem(lax.div(s, 2), XR)

        @pl.when(rel == 0)
        def _():
            load_own(k, slot, half).start()

        @pl.when(rel > 0)
        def _():
            remote(xall.at[rel, k], xall.at[rel, k], so_x.at[0, 0], rx_sem.at[rel, k], partner).wait_recv()
            remote(vt.at[rel, k], vt.at[rel, k], so_v.at[0, 0], rv_sem.at[rel, k], partner).wait_recv()
            pltpu.make_async_copy(
                xall.at[rel, k], xr.at[slot, pl.ds(half * T, T)], ld_sem.at[slot, half]
            ).start()

        @pl.when(jnp.logical_and(rel >= 2, lax.rem(rel, 2) == 0))
        def _():
            for copy in forward_partner(rel, k):
                copy.start()

        @pl.when(jnp.logical_and(rel == 2, lax.rem(k, 2) == 1))
        def _():
            for copy in forward_nbr(2, k, nbr_y):
                copy.start()

        @pl.when(jnp.logical_and(rel == 4, lax.rem(k, 2) == 0))
        def _():
            for copy in forward_nbr(4, k, nbr_x):
                copy.start()

    def trip(t, parity, place):
        if place < 2:
            fetch(2 * t + 2)
            fetch(2 * t + 3)
        if place > 0:
            write_k(t - 1, 1 - parity)

            @pl.when(t >= 2)
            def _():
                written(parity)

        x_slot = parity
        load_own(0, x_slot, 0).wait()
        load_own(0, x_slot, 1).wait()
        for p in range(2 * NP):
            rows = slice(p * PIECE, (p + 1) * PIECE)
            part = xr[x_slot, rows, :].astype(jnp.float32)
            norm = jnp.sum(part * part, axis=1, keepdims=True)
            nj[rows, :] = jnp.broadcast_to(norm, (PIECE, 128))
        if place > 0:
            lhs = pair_of(vt, t - 1)
        for i in range(NCH + 4):
            if place > 0 and i >= 4:
                apply(stage, 1 - parity, lhs, i - 4)
            if i < NCH:
                weigh(x_slot, parity, i)

    trip(jnp.int32(0), 0, 0)

    @pl.loop(0, PAIRS // 2 - 1)
    def _(m):
        trip(2 * m + 1, 1, 1)
        trip(2 * m + 2, 0, 1)

    trip(jnp.int32(PAIRS - 1), 1, 2)
    write_k(jnp.int32(PAIRS - 1), 1)
    written(0)
    for number in (0, 2):
        read_k(jnp.int32(number), number).start()
    lhs = pair_of(vt, jnp.int32(PAIRS - 1))
    for i in range(NCH):
        apply(stage, 1, lhs, i)

    @pl.loop(0, NCH)
    def _(k):
        yall[0, k] = ysum[k].astype(jnp.bfloat16)

    @pl.loop(0, NCH)
    def _(k):
        ysum[k] = jnp.zeros((COLS, T), jnp.float32)

    written(1)
    read_k(jnp.int32(1), 1).start()
    half = NCH // 2

    def y_copy(src_rel, dst_rel, lo, n, idx, dev):
        return remote(
            yall.at[src_rel, pl.ds(lo, n)], yall.at[dst_rel, pl.ds(lo, n)], ys_sem.at[idx], yr_sem.at[idx], dev
        )

    y_moves = (
        (0, 1, 0, NCH, partner),
        (0, 2, 0, NCH, nbr_x),
        (0, 4, 0, NCH, nbr_y),
        (2, 3, 0, NCH, partner),
        (4, 5, 0, NCH, partner),
        (4, 6, 0, half, nbr_x),
        (2, 6, half, half, nbr_y),
        (6, 7, 0, NCH, partner),
    )

    def y_move(idx):
        src, dst, lo, n, dev = y_moves[idx]
        return y_copy(src, dst, lo, n, idx, dev)

    def y_arrived(idx):
        _, dst, lo, n, dev = y_moves[idx]
        return y_copy(dst, dst, lo, n, idx, dev)

    for idx in range(3):
        y_move(idx).start()

    def use(t, source, slot):
        lhs = pair_of(yall, t)
        for i in range(NCH):
            apply(source, slot, lhs, i)

    def use_streamed(t, number, slot):
        read_k(number, slot).wait()
        use(t, stage, slot)

        @pl.when(number + RING < N_STREAM)
        def _():
            read_k(number + RING, slot).start()

    def use_first(lo, hi):
        @pl.loop(lo, hi)
        def _(m):
            @pl.when(m == 2)
            def _():
                y_arrived(0).wait_recv()

            for slot in range(RING):
                use_streamed(RING * m + slot, RING * m + slot, slot)

    use_first(0, 3)
    y_arrived(1).wait_recv()
    y_arrived(2).wait_recv()
    for idx in range(3, 7):
        y_move(idx).start()
    @pl.loop(0, NCH)
    def _(k):
        for which, dev in enumerate((partner, nbr_x, nbr_y)):
            for copy in send_own(k, which, dev):
                copy.wait_send()
        for rel in (2, 4, 6):
            for copy in forward_partner(rel, k):
                copy.wait_send()
        for copy in forward_nbr(2, k, nbr_y):
            copy.wait_send()

    use_first(3, 4)
    y_arrived(3).wait_recv()
    y_arrived(4).wait_recv()

    @pl.loop(0, (PAIRS - 12) // RES_OF)
    def _(o):
        @pl.when(o == 3)
        def _():
            y_arrived(5).wait_recv()
            y_arrived(6).wait_recv()
            y_move(7).start()

        @pl.when(o == 5)
        def _():
            y_arrived(7).wait_recv()

        t = 12 + o * RES_OF
        for slot in range(RING):
            use_streamed(t + RES_IN + slot, 12 + o * RING + slot, slot)
            if slot < RES_IN:
                use(t + slot, kept, o * RES_IN + slot)

    use_streamed(jnp.int32(PAIRS - 1), jnp.int32(N_STREAM - 1), 0)

    for idx in range(8):
        y_move(idx).wait_send()

    @pl.loop(0, NCH)
    def _(k):
        out_ref[k] = ysum[k]


def solution(mesh):
    rows = NCH * T

    def local_program(x_loc, v_loc, length_scale, out_scale):
        vt_loc = v_loc.reshape(NCH, T, COLS).transpose(0, 2, 1)
        dma = pltpu.SemaphoreType.DMA
        out, _, _ = pl.pallas_call(
            body,
            out_shape=(
                jax.ShapeDtypeStruct((NCH, COLS, T), jnp.float32),
                jax.ShapeDtypeStruct((NREL, NCH, T, FEAT), jnp.bfloat16),
                jax.ShapeDtypeStruct((N_STREAM, NCH, 2, 2 * T, 128), jnp.bfloat16),
            ),
            in_specs=[
                pl.BlockSpec(memory_space=pltpu.HBM),
                pl.BlockSpec(memory_space=pltpu.HBM),
                pl.BlockSpec(memory_space=pltpu.SMEM),
                pl.BlockSpec(memory_space=pltpu.SMEM),
            ],
            out_specs=(
                pl.BlockSpec(memory_space=pltpu.VMEM),
                pl.BlockSpec(memory_space=pltpu.HBM),
                pl.BlockSpec(memory_space=pltpu.HBM),
            ),
            scratch_shapes=[
                pltpu.VMEM((NCH, 2, FEAT, 128), jnp.bfloat16),
                pltpu.VMEM((NREL, NCH, COLS, T), jnp.bfloat16),
                pltpu.VMEM((NREL, NCH, COLS, T), jnp.bfloat16),
                pltpu.VMEM((N_RES, NCH, 2, 2 * T, 128), jnp.bfloat16),
                pltpu.VMEM((RING, NCH, 2, 2 * T, 128), jnp.bfloat16),
                pltpu.VMEM((XR, 2 * T, FEAT), jnp.bfloat16),
                pltpu.VMEM((2 * T, 128), jnp.float32),
                pltpu.VMEM((NCH, 8, T), jnp.float32),
                dma((XR, 2)), dma((2,)), dma((RING,)), dma,
                dma((NREL, NCH)), dma((NREL, NCH)),
                dma((3, NCH)), dma((3, NCH)),
                dma((3, NCH)), dma((3, NCH)),
                dma((NCH,)), dma((NCH,)),
                dma((8,)), dma((8,)),
                pltpu.VMEM((NCH, COLS, T), jnp.float32),
                pltpu.VMEM((2, 8, 128), jnp.float32),
                dma((NCH,)),
            ],
            compiler_params=pltpu.CompilerParams(
                collective_id=0,
                has_side_effects=True,
                vmem_limit_bytes=67_043_328
            ),
        )(x_loc.reshape(NCH, T, FEAT), vt_loc, length_scale, out_scale)
        return out.transpose(0, 2, 1).reshape(rows, COLS)

    row_spec = P(("task", "row"), None)
    return jax.shard_map(
        local_program,
        mesh=mesh,
        in_specs=(row_spec, row_spec, P("task"), P("task")),
        out_specs=row_spec,
        check_vma=False,
    )
```

```python
import functools
import math

import jax
import jax.numpy as jnp
from jax import lax
from jax.experimental import pallas as pl
from jax.experimental.pallas import tpu as pltpu
from jax.sharding import PartitionSpec as P

MESH = pl.DeviceIdType.MESH
T = 256
FEAT = 512
COLS = 64
NCH = 12
NREL = 8
STEPS = NREL * NCH
PIECE = 64
NP = T // PIECE
NI = NCH // 2
PAIRS = STEPS // 2
RES_IN, RES_OF = 2, 5
N_RES = (PAIRS - 12) // RES_OF * RES_IN
RING = 3
N_STREAM = PAIRS - N_RES
XR = 2


def split(n, by, factor, power):
    whole = lax.div(n * factor, power)
    return whole, n - whole * by


def chunk_of(s):
    j = lax.rem(s + 2, 4)
    v = lax.div(s - 22, 4) - 1
    late = jnp.where(s < 26, 0, jnp.where(s >= 94, 1, lax.div(j, 2)))
    group = jnp.where(s < 26, 0, jnp.where(s >= 94, 17, v + 1 - late))
    side = lax.rem(s, 2)
    far = group >= 12
    rel = jnp.where(far, 6, 2 + 2 * side) + late
    chunk = jnp.where(far, 2 * (group - 12) + side, group)
    near_rel, near_chunk = split(s, NCH, 43, 512)
    return jnp.where(s < 24, near_rel, rel), jnp.where(s < 24, near_chunk, chunk)


def wide(left, right):
    return jnp.concatenate([left, right], axis=1)


def stream_of(t):
    u = jnp.maximum(t - 12, 0)
    o, w = split(u, RES_OF, 205, 1024)
    keep = jnp.where(o == (PAIRS - 12) // RES_OF, 0, RES_IN)
    streamed = jnp.logical_or(t < 12, w >= keep)
    number = jnp.where(t < 12, t, 12 + o * (RES_OF - RES_IN) + w - keep)
    return streamed, number, o * RES_IN + w


def body(
    x_hbm, vt_hbm, ls_ref, os_ref,
    out_ref, xall, kst,
    xt, vt, yall, kept, stage, xr, nj, ni,
    ld_sem, kw_sem, kr_sem, vl_sem,
    rx_sem, rv_sem, so_x, so_v, sp_x, sp_v, sn_x, sn_v, ys_sem, yr_sem,
    ysum, consts, su_sem,
):
    me = lax.axis_index("row")
    partner = me + 1 - 2 * lax.rem(me, 2)
    nbr_x = me + 2 - 4 * lax.rem(lax.div(me, 2), 2)
    nbr_y = me + 4 - 8 * lax.div(me, 4)

    def remote(src, dst, ss, rs, dev):
        return pltpu.make_async_remote_copy(
            src_ref=src, dst_ref=dst, send_sem=ss, recv_sem=rs, device_id={"row": dev}, device_id_type=MESH
        )

    def send_own(k, which, dev):
        slot = (1, 2, 4)[which]
        return (
            remote(x_hbm.at[k], xall.at[slot, k], so_x.at[which, k], rx_sem.at[slot, k], dev),
            remote(vt_hbm.at[k], vt.at[slot, k], so_v.at[which, k], rv_sem.at[slot, k], dev),
        )

    def forward_partner(rel, k):
        row = lax.div(rel, 2) - 1
        return (
            remote(xall.at[rel, k], xall.at[rel + 1, k], sp_x.at[row, k], rx_sem.at[rel + 1, k], partner),
            remote(vt.at[rel, k], vt.at[rel + 1, k], sp_v.at[row, k], rv_sem.at[rel + 1, k], partner),
        )

    def forward_nbr(rel, k, dev):
        return (
            remote(xall.at[rel, k], xall.at[6, k], sn_x.at[k], rx_sem.at[6, k], dev),
            remote(vt.at[rel, k], vt.at[6, k], sn_v.at[k], rv_sem.at[6, k], dev),
        )

    barrier = pltpu.get_barrier_semaphore()
    for dev in (partner, nbr_x, nbr_y):
        pl.semaphore_signal(barrier, inc=1, device_id={"row": dev}, device_id_type=MESH)

    own_v = pltpu.make_async_copy(vt_hbm, vt.at[0], vl_sem)
    own_v.start()

    def load_own(k, slot, half):
        return pltpu.make_async_copy(x_hbm.at[k], xr.at[slot, pl.ds(half * T, T)], ld_sem.at[slot, half])

    @pl.loop(0, NCH)
    def _(k):
        for q in range(4):
            pltpu.make_async_copy(
                x_hbm.at[k, :, pl.ds(q * 128, 128)],
                stage.at[RING - 1, k, q // 2, pl.ds(q % 2 * T, T)],
                su_sem.at[k],
            ).start()

    load_own(0, 0, 0).start()
    load_own(1, 0, 1).start()
    pl.semaphore_wait(barrier, 3)

    @pl.loop(0, NCH)
    def _(k):
        for which, dev in enumerate((partner, nbr_x, nbr_y)):
            for copy in send_own(k, which, dev):
                copy.start()

    @pl.loop(0, NCH)
    def _(k):
        pltpu.make_async_copy(x_hbm.at[k], xr.at[1, pl.ds(0, T)], su_sem.at[k]).wait()
        norm = jnp.zeros((1, T), jnp.float32)
        for q in range(4):
            part = stage[RING - 1, k, q // 2, q % 2 * T : (q % 2 + 1) * T, :].astype(jnp.float32).T
            norm = norm + jnp.sum(part * part, axis=0, keepdims=True)
            scaled = (part * -2.0).astype(jnp.bfloat16)
            for side in range(2):
                xt[k, side, q * 128 : (q + 1) * 128, :] = scaled[:, side * 128 : (side + 1) * 128]
        ni[k] = jnp.broadcast_to(norm, (8, T))

    own_v.wait()

    scale = jnp.full((8, 128), ls_ref[0], jnp.float32)
    consts[0] = -math.log2(math.e) / (2.0 * scale * scale)
    consts[1] = jnp.full((8, 128), os_ref[0], jnp.float32)

    @pl.loop(0, NCH)
    def _(k):
        ysum[k] = jnp.zeros((COLS, T), jnp.float32)

    def write_k(t, parity):
        streamed, number, slot = stream_of(t)

        @pl.when(streamed)
        def _():
            pltpu.make_async_copy(stage.at[parity], kst.at[number], kw_sem.at[parity]).start()

        @pl.when(jnp.logical_not(streamed))
        def _():
            pltpu.make_async_copy(stage.at[parity], kept.at[slot], kw_sem.at[parity]).start()

    def written(parity):
        pltpu.make_async_copy(stage.at[parity], kst.at[0], kw_sem.at[parity]).wait()

    def read_k(number, slot):
        return pltpu.make_async_copy(kst.at[number], stage.at[slot], kr_sem.at[slot])

    def weigh(x_slot, parity, i):
        if i % 2:
            return
        both = wide(wide(xt[i, 0], xt[i, 1]), wide(xt[i + 1, 0], xt[i + 1, 1]))
        for c in range(2):
            rows = slice(c * 256, (c + 1) * 256)
            tiles = jnp.dot(xr[x_slot, rows, :], both, preferred_element_type=jnp.float32)
            finish(tiles[:, :T], parity, i, rows)
            finish(tiles[:, T:], parity, i + 1, rows)

    def finish(gram_tile, parity, i, rows):
        for h in range(2):
            lanes = slice(h * 128, (h + 1) * 128)
            dist = jnp.maximum((nj[rows, :] + ni[i, 0:1, lanes]) + gram_tile[:, lanes], 0.0)
            stage[parity, i, h, rows] = (consts[1, 0:1, :] * jnp.exp2(dist * consts[0, 0:1, :])).astype(jnp.bfloat16)

    def apply(source, slot, lhs, i):
        ysum[i] += jnp.dot(lhs, wide(source[slot, i, 0], source[slot, i, 1]), preferred_element_type=jnp.float32)

    def pair_of(table, t):
        rel, k = chunk_of(2 * t)
        rel_2, k_2 = chunk_of(2 * t + 1)
        return jnp.concatenate([table[rel, k], table[rel_2, k_2]], axis=1)

    def fetch(s):
        rel, k = chunk_of(s)
        half = lax.rem(s, 2)
        slot = lax.rem(lax.div(s, 2), XR)

        @pl.when(rel == 0)
        def _():
            load_own(k, slot, half).start()

        @pl.when(rel > 0)
        def _():
            remote(xall.at[rel, k], xall.at[rel, k], so_x.at[0, 0], rx_sem.at[rel, k], partner).wait_recv()
            remote(vt.at[rel, k], vt.at[rel, k], so_v.at[0, 0], rv_sem.at[rel, k], partner).wait_recv()
            pltpu.make_async_copy(
                xall.at[rel, k], xr.at[slot, pl.ds(half * T, T)], ld_sem.at[slot, half]
            ).start()

        @pl.when(jnp.logical_and(rel >= 2, lax.rem(rel, 2) == 0))
        def _():
            for copy in forward_partner(rel, k):
                copy.start()

        @pl.when(jnp.logical_and(rel == 2, lax.rem(k, 2) == 1))
        def _():
            for copy in forward_nbr(2, k, nbr_y):
                copy.start()

        @pl.when(jnp.logical_and(rel == 4, lax.rem(k, 2) == 0))
        def _():
            for copy in forward_nbr(4, k, nbr_x):
                copy.start()

    def trip(t, parity, place):
        if place > 0:
            write_k(t - 1, 1 - parity)
        if place < 2:
            fetch(2 * t + 2)
            fetch(2 * t + 3)
        if place > 0:

            @pl.when(t >= 2)
            def _():
                written(parity)

        x_slot = parity
        load_own(0, x_slot, 0).wait()
        load_own(0, x_slot, 1).wait()
        for p in range(2 * NP):
            rows = slice(p * PIECE, (p + 1) * PIECE)
            part = xr[x_slot, rows, :].astype(jnp.float32)
            norm = jnp.sum(part * part, axis=1, keepdims=True)
            nj[rows, :] = jnp.broadcast_to(norm, (PIECE, 128))
        if place > 0:
            lhs = pair_of(vt, t - 1)
        for i in range(NCH + 6):
            if place > 0 and i >= 6:
                apply(stage, 1 - parity, lhs, i - 6)
            if i < NCH:
                weigh(x_slot, parity, i)

    trip(jnp.int32(0), 0, 0)

    @pl.loop(0, PAIRS // 2 - 1)
    def _(m):
        trip(2 * m + 1, 1, 1)
        trip(2 * m + 2, 0, 1)

    trip(jnp.int32(PAIRS - 1), 1, 2)
    write_k(jnp.int32(PAIRS - 1), 1)
    written(0)
    for number in (0, 2):
        read_k(jnp.int32(number), number).start()
    lhs = pair_of(vt, jnp.int32(PAIRS - 1))
    for i in range(NCH):
        apply(stage, 1, lhs, i)

    @pl.loop(0, NCH)
    def _(k):
        yall[0, k] = ysum[k].astype(jnp.bfloat16)

    @pl.loop(0, NCH)
    def _(k):
        ysum[k] = jnp.zeros((COLS, T), jnp.float32)

    written(1)
    read_k(jnp.int32(1), 1).start()
    half = NCH // 2

    def y_copy(src_rel, dst_rel, lo, n, idx, dev):
        return remote(
            yall.at[src_rel, pl.ds(lo, n)], yall.at[dst_rel, pl.ds(lo, n)], ys_sem.at[idx], yr_sem.at[idx], dev
        )

    y_moves = (
        (0, 1, 0, NCH, partner),
        (0, 2, 0, NCH, nbr_x),
        (0, 4, 0, NCH, nbr_y),
        (2, 3, 0, NCH, partner),
        (4, 5, 0, NCH, partner),
        (4, 6, 0, half, nbr_x),
        (2, 6, half, half, nbr_y),
        (6, 7, 0, NCH, partner),
    )

    def y_move(idx):
        src, dst, lo, n, dev = y_moves[idx]
        return y_copy(src, dst, lo, n, idx, dev)

    def y_arrived(idx):
        _, dst, lo, n, dev = y_moves[idx]
        return y_copy(dst, dst, lo, n, idx, dev)

    for idx in range(3):
        y_move(idx).start()

    def use(t, source, slot):
        lhs = pair_of(yall, t)
        for i in range(NCH):
            apply(source, slot, lhs, i)

    def use_streamed(t, number, slot):
        read_k(number, slot).wait()
        use(t, stage, slot)

        @pl.when(number + RING < N_STREAM)
        def _():
            read_k(number + RING, slot).start()

    def use_first(lo, hi):
        @pl.loop(lo, hi)
        def _(m):
            @pl.when(m == 2)
            def _():
                y_arrived(0).wait_recv()

            for slot in range(RING):
                use_streamed(RING * m + slot, RING * m + slot, slot)

    use_first(0, 3)
    y_arrived(1).wait_recv()
    y_arrived(2).wait_recv()
    for idx in range(3, 7):
        y_move(idx).start()
    @pl.loop(0, NCH)
    def _(k):
        for which, dev in enumerate((partner, nbr_x, nbr_y)):
            for copy in send_own(k, which, dev):
                copy.wait_send()
        for rel in (2, 4, 6):
            for copy in forward_partner(rel, k):
                copy.wait_send()
        for copy in forward_nbr(2, k, nbr_y):
            copy.wait_send()

    use_first(3, 4)
    y_arrived(3).wait_recv()
    y_arrived(4).wait_recv()

    @pl.loop(0, (PAIRS - 12) // RES_OF)
    def _(o):
        @pl.when(o == 3)
        def _():
            y_arrived(5).wait_recv()
            y_arrived(6).wait_recv()
            y_move(7).start()

        @pl.when(o == 5)
        def _():
            y_arrived(7).wait_recv()

        t = 12 + o * RES_OF
        for slot in range(RING):
            use_streamed(t + RES_IN + slot, 12 + o * RING + slot, slot)
            if slot < RES_IN:
                use(t + slot, kept, o * RES_IN + slot)

    use_streamed(jnp.int32(PAIRS - 1), jnp.int32(N_STREAM - 1), 0)

    for idx in range(8):
        y_move(idx).wait_send()

    @pl.loop(0, NCH)
    def _(k):
        out_ref[k] = ysum[k]


def solution(mesh):
    rows = NCH * T

    def local_program(x_loc, v_loc, length_scale, out_scale):
        vt_loc = v_loc.reshape(NCH, T, COLS).transpose(0, 2, 1)
        dma = pltpu.SemaphoreType.DMA
        out, _, _ = pl.pallas_call(
            body,
            out_shape=(
                jax.ShapeDtypeStruct((NCH, COLS, T), jnp.float32),
                jax.ShapeDtypeStruct((NREL, NCH, T, FEAT), jnp.bfloat16),
                jax.ShapeDtypeStruct((N_STREAM, NCH, 2, 2 * T, 128), jnp.bfloat16),
            ),
            in_specs=[
                pl.BlockSpec(memory_space=pltpu.HBM),
                pl.BlockSpec(memory_space=pltpu.HBM),
                pl.BlockSpec(memory_space=pltpu.SMEM),
                pl.BlockSpec(memory_space=pltpu.SMEM),
            ],
            out_specs=(
                pl.BlockSpec(memory_space=pltpu.VMEM),
                pl.BlockSpec(memory_space=pltpu.HBM),
                pl.BlockSpec(memory_space=pltpu.HBM),
            ),
            scratch_shapes=[
                pltpu.VMEM((NCH, 2, FEAT, 128), jnp.bfloat16),
                pltpu.VMEM((NREL, NCH, COLS, T), jnp.bfloat16),
                pltpu.VMEM((NREL, NCH, COLS, T), jnp.bfloat16),
                pltpu.VMEM((N_RES, NCH, 2, 2 * T, 128), jnp.bfloat16),
                pltpu.VMEM((RING, NCH, 2, 2 * T, 128), jnp.bfloat16),
                pltpu.VMEM((XR, 2 * T, FEAT), jnp.bfloat16),
                pltpu.VMEM((2 * T, 128), jnp.float32),
                pltpu.VMEM((NCH, 8, T), jnp.float32),
                dma((XR, 2)), dma((2,)), dma((RING,)), dma,
                dma((NREL, NCH)), dma((NREL, NCH)),
                dma((3, NCH)), dma((3, NCH)),
                dma((3, NCH)), dma((3, NCH)),
                dma((NCH,)), dma((NCH,)),
                dma((8,)), dma((8,)),
                pltpu.VMEM((NCH, COLS, T), jnp.float32),
                pltpu.VMEM((2, 8, 128), jnp.float32),
                dma((NCH,)),
            ],
            compiler_params=pltpu.CompilerParams(
                collective_id=0,
                has_side_effects=True,
                vmem_limit_bytes=67_043_328
            ),
        )(x_loc.reshape(NCH, T, FEAT), vt_loc, length_scale, out_scale)
        return out.transpose(0, 2, 1).reshape(rows, COLS)

    row_spec = P(("task", "row"), None)
    return jax.shard_map(
        local_program,
        mesh=mesh,
        in_specs=(row_spec, row_spec, P("task"), P("task")),
        out_specs=row_spec,
        check_vma=False,
    )
```
